256 devices in a mesh: leaf: 64 (over z, x, core), blk: 4 (over y).
Axes of the slice: x: 4, y: 4, z: 8, core: 2. Of those that a mesh axis runs over, the one named last changes fastest.
Arguments:
- desc_panel: bfloat16 [16384, 384, 128], P(('leaf', 'blk')), may hold values from -18 to 18
- row_map: int32 [16384, 3], P(('leaf', 'blk')), may hold values from 0 to 279, as said below
- anc_order: int32 [64], replicated, may hold values from 0 to 63, as said below
- anc_below: int32 [64, 12], replicated, may hold values from 256 to 279, as said below
- anc_panel: float32 [64, 4, 4, 128, 512], P('leaf', None, 'blk'), may hold values from -6 to 27, as said below
Outputs:
- chol_panel: float32 [64, 4, 4, 128, 512], P('leaf', None, 'blk')
The draws below stay inside these ranges and needn't reach their ends.
Inputs may be any that keep to these rules, and one draw needn't show every extreme that they name: `row_map`: entry 0 of each row is a column block of one ancestor; the other entries are distinct entries of that ancestor's row of anc_below. Over the descendants of one device, entry 0 names the column blocks of any one ancestor at most 2 times, and of some ancestor exactly 2 times. `anc_order`: each leaf index holds a different column range. `anc_below`: each row holds 12 distinct indices. `anc_panel`: the leading 512 rows of each ancestor's panel are symmetric, and the leading block of S stays positive definite.
All inputs are finite; a program needn't handle non-finite values.
Results may differ from the reference program's by a relative error of at most 0.0003.
Values may be sent and summed in bfloat16 or wider, within the bound.
A program may use at most 192 MiB of HBM per device.

```python
import jax
import jax.numpy as jnp
from jax import lax

BR = 128
WD = 128
CB = 4
W = 512
Q = 12
P_SIZE = 16
EXTRA = 24
RB = 3
NA = 64
DESC_DEV = 64
ND = 16384
N_BLK = 4


def tree_structure(key):
    keys = jax.random.split(jax.random.fold_in(key, 41), 5)
    anc_order = jax.random.permutation(keys[0], NA).astype(jnp.int32)
    below_picks = jax.vmap(lambda k: jax.random.permutation(k, EXTRA)[:Q])(jax.random.split(keys[1], NA))
    anc_below = (below_picks + NA * CB).astype(jnp.int32)
    device_count = ND // DESC_DEV
    quarter = NA // 4

    def device_targets(k):
        first_key, second_key = jax.random.split(k)
        order = jax.random.permutation(first_key, NA)
        listed = jnp.concatenate([order[:quarter], order[:quarter], order[quarter:3 * quarter]])
        return listed[jax.random.permutation(second_key, DESC_DEV)]
    targets = jax.vmap(device_targets)(jax.random.split(keys[2], device_count)).reshape(ND).astype(jnp.int32)
    columns = jax.random.randint(keys[3], (ND,), 0, CB).astype(jnp.int32)
    picks = jax.vmap(lambda k: jax.random.permutation(k, Q)[:RB - 1])(jax.random.split(keys[4], ND)).astype(jnp.int32)
    below = jnp.take_along_axis(anc_below[targets], picks, axis=1)
    head = anc_order[targets] * CB + columns
    row_map = jnp.concatenate([head[:, None], below], axis=1).astype(jnp.int32)
    return (anc_order, anc_below, row_map)


def draw_anc_order(key, part):
    return tree_structure(key)[0]


def draw_anc_below(key, part):
    return tree_structure(key)[1]


def draw_row_map(key, part):
    return tree_structure(key)[2]


def draw_desc_panel(key, part):
    key = jax.random.fold_in(key, 31)
    shape = (ND, RB, BR, WD)
    values = jnp.clip(jax.random.normal(key, shape, jnp.float32), -6.0, 6.0)
    device_count = ND // DESC_DEV
    head_scale = (2.0 * CB / (device_count * WD)) ** 0.5
    scales = jnp.where(jnp.arange(RB) < 1, head_scale, 3.0).astype(jnp.float32)
    return (values * scales[None, :, None, None]).reshape(ND, RB * BR, WD).astype(jnp.bfloat16)


def draw_anc_panel(key, part):
    keys = jax.random.split(jax.random.fold_in(key, 23), 2)
    total_rows = P_SIZE * BR
    noise = jnp.clip(jax.random.normal(keys[0], (NA, total_rows, W), jnp.float32), -6.0, 6.0)
    diagonal = jax.random.uniform(keys[1], (NA, W), jnp.float32, 12.0, 24.0)
    upper = noise[:, :W, :] * (1.5 / W ** 0.5)
    symmetric = (upper + jnp.swapaxes(upper, 1, 2)) / 2.0 ** 0.5
    symmetric = symmetric + diagonal[:, :, None] * jnp.eye(W, dtype=jnp.float32)[None, :, :]
    whole = jnp.concatenate([symmetric, noise[:, W:, :]], axis=1)
    return whole.reshape(NA, P_SIZE // N_BLK, N_BLK, BR, W).astype(jnp.float32)


def setup_inputs(seed: int = 0) -> dict:
    seeds = jax.random.split(jax.random.key(seed), 6)
    return {
        "desc_panel": draw_desc_panel(jax.random.fold_in(seeds[5], 71), 0),
        "row_map": draw_row_map(jax.random.fold_in(seeds[5], 71), 0),
        "anc_order": draw_anc_order(jax.random.fold_in(seeds[5], 71), 0),
        "anc_below": draw_anc_below(jax.random.fold_in(seeds[5], 71), 0),
        "anc_panel": draw_anc_panel(jax.random.fold_in(seeds[5], 71), 0),
    }


def structure_positions(block_ids, owner_leaf, anc_order, anc_below):
    column_base = anc_order[owner_leaf] * CB
    relative = block_ids - column_base[:, None]
    in_columns = (relative >= 0) & (relative < CB)
    below_ids = anc_below[owner_leaf]
    matching = block_ids[:, :, None] == below_ids[:, None, :]
    offsets = CB + jnp.arange(Q, dtype=jnp.int32)
    below_place = jnp.sum(jnp.where(matching, offsets[None, None, :], 0), axis=2)
    located = jnp.any(matching, axis=2)
    return jnp.where(in_columns, relative, jnp.where(located, below_place, P_SIZE)).astype(jnp.int32)

def owner_of(ranges, anc_order):
    leaves = jnp.arange(NA, dtype=jnp.int32)
    return jnp.sum(jnp.where(anc_order[None, :] == ranges[:, None], leaves[None, :], 0), axis=1).astype(jnp.int32)

def reference(desc_panel, row_map, anc_order, anc_below, anc_panel):
    device_count = ND // DESC_DEV
    panel_groups = desc_panel.reshape(device_count, DESC_DEV, RB, BR, WD)
    id_groups = row_map.reshape(device_count, DESC_DEV, RB)

    def absorb(running, element):
        panel_block, block_ids = element
        blocks = panel_block.astype(jnp.float32)
        owner_leaf = owner_of(block_ids[:, 0] // CB, anc_order)
        positions = structure_positions(block_ids, owner_leaf, anc_order, anc_below)
        column = (block_ids[:, 0] % CB).astype(jnp.int32)
        product = jnp.einsum('nrxw,nyw->nrxy', blocks, blocks[:, 0], precision=lax.Precision.HIGHEST)
        running = running.at[owner_leaf[:, None], positions, :, column[:, None], :].add(product)
        return (running, None)
    initial = jnp.zeros((NA, P_SIZE + 1, BR, CB, BR), jnp.float32)
    running, _ = lax.scan(absorb, initial, (panel_groups, id_groups))
    update = running[:, :P_SIZE].reshape(NA, P_SIZE * BR, W)
    schur_rows = anc_panel.reshape(NA, P_SIZE * BR, W) - update

    def factor(panel_rows):
        lower_factor = jnp.linalg.cholesky(panel_rows[:W])
        return jax.scipy.linalg.solve_triangular(lower_factor, panel_rows.T, lower=True).T
    return lax.map(factor, schur_rows).reshape(anc_panel.shape)
```

```python
import functools

import jax
import jax.numpy as jnp
from jax import lax
from jax.experimental import pallas as pl
from jax.experimental.pallas import tpu as pltpu
from jax.sharding import Mesh
from jax.sharding import PartitionSpec as P

Z, XC, Y = 8, 8, 4
PLANE = XC * Y
BR = 128
CB = 4
Q = 12
SLOTS = 2
NA = 64
NONE = 7
META = 16
HEAD_ROWS = 2 * SLOTS * BR + META
BELOW = Q * CB
HIGHEST = lax.Precision.HIGHEST
ALL = ("z", "xc", "y")


def nt_dot(a, b, precision=None):
    return lax.dot_general(
        a, b, (((1,), (1,)), ((), ())), precision=precision, preferred_element_type=jnp.float32
    )


def pack_kernel(
    map_ref, order_ref, below_ref, desc_ref, head_ref, tail0_ref, tail1_ref,
    stage, meta, inverse, used, codes, in_sems, head_sem, tail_sem, meta_sem,
):
    count = map_ref.shape[0]
    parts = in_sems.shape[0]
    step = count // parts

    def load(k):
        part = pl.ds(k * step, step)
        return pltpu.make_async_copy(desc_ref.at[part], stage.at[part], in_sems.at[k])

    for k in range(parts):
        load(k).start()

    def clear(a, carry):
        inverse[order_ref[a]] = a
        used[a] = 0
        for s in range(SLOTS):
            codes[(a * SLOTS + s) * 4] = NONE
            codes[(a * SLOTS + s) * 4 + 1] = 0
            codes[(a * SLOTS + s) * 4 + 2] = 0
        return carry

    lax.fori_loop(0, NA, clear, 0)

    def route(d, carry):
        head = map_ref[d, 0]
        a = inverse[head // CB]
        s = used[a]
        used[a] = s + 1
        dest = (a % XC) * Y + (a // XC) % Y
        i = jnp.bitwise_xor(a // (XC * Y), a % 2)
        slot = (dest * 2 + i) * SLOTS + s
        first, second = map_ref[d, 1], map_ref[d, 2]
        j1, j2 = jnp.int32(0), jnp.int32(0)
        for j in range(Q):
            g = below_ref[a, j]
            j1 = jnp.where(g == first, j, j1)
            j2 = jnp.where(g == second, j, j2)
        codes[slot * 4] = head % CB
        codes[slot * 4 + 1] = j1
        codes[slot * 4 + 2] = j2
        codes[NA * SLOTS * 4 + d] = slot
        return carry

    lax.fori_loop(0, count, route, 0)

    lane = lax.broadcasted_iota(jnp.int32, (META, 128), 1)

    def describe(dest, carry):
        row = jnp.zeros((META, 128), jnp.int32)
        for t in range(2 * SLOTS):
            for f in range(3):
                row = jnp.where(lane == t * 3 + f, codes[(dest * 2 * SLOTS + t) * 4 + f], row)
        meta[dest] = row.astype(jnp.float32).astype(jnp.bfloat16)
        return carry

    lax.fori_loop(0, PLANE, describe, 0)

    for k in range(parts):
        load(k).wait()

    def send_head(d, carry):
        slot = codes[NA * SLOTS * 4 + d]
        place = pl.multiple_of((slot % (2 * SLOTS)) * BR, BR)
        pltpu.make_async_copy(
            stage.at[d, pl.ds(0, BR)],
            head_ref.at[slot // (2 * SLOTS), pl.ds(place, BR)],
            head_sem,
        ).start()
        return carry

    lax.fori_loop(0, count, send_head, 0)
    pltpu.make_async_copy(meta, head_ref.at[:, pl.ds(2 * SLOTS * BR, META)], meta_sem).start()

    def send_tail(d, carry):
        slot = codes[NA * SLOTS * 4 + d]
        dest, i, s = slot // (2 * SLOTS), (slot // SLOTS) % 2, slot % SLOTS
        for k, out in ((0, tail0_ref), (1, tail1_ref)):
            @pl.when(i == k)
            def _():
                pltpu.make_async_copy(
                    stage.at[d, pl.ds(BR, 2 * BR)], out.at[dest, s], tail_sem
                ).start()
        return carry

    lax.fori_loop(0, count, send_tail, 0)
    pltpu.make_async_copy(meta, head_ref.at[:, pl.ds(2 * SLOTS * BR, META)], meta_sem).wait()
    heads = stage.at[:, pl.ds(0, BR)]
    pltpu.make_async_copy(heads, heads, head_sem).wait()
    tails = stage.at[:, pl.ds(BR, 2 * BR)]
    pltpu.make_async_copy(tails, tails, tail_sem).wait()


def pack(row_map, anc_order, anc_below, desc_panel):
    count = row_map.shape[0]
    smem = pl.BlockSpec(memory_space=pltpu.SMEM)
    hbm = pl.BlockSpec(memory_space=pltpu.HBM)
    dt = desc_panel.dtype
    return pl.pallas_call(
        pack_kernel,
        out_shape=(
            jax.ShapeDtypeStruct((PLANE, HEAD_ROWS, BR), dt),
            jax.ShapeDtypeStruct((PLANE, SLOTS, 2 * BR, BR), dt),
            jax.ShapeDtypeStruct((PLANE, SLOTS, 2 * BR, BR), dt),
        ),
        in_specs=[smem, smem, smem, hbm],
        out_specs=(hbm, hbm, hbm),
        scratch_shapes=[
            pltpu.VMEM(desc_panel.shape, dt),
            pltpu.VMEM((PLANE, META, BR), dt),
            pltpu.SMEM((NA,), jnp.int32),
            pltpu.SMEM((NA,), jnp.int32),
            pltpu.SMEM((NA * SLOTS * 4 + count,), jnp.int32),
            pltpu.SemaphoreType.DMA((4,)),
            pltpu.SemaphoreType.DMA,
            pltpu.SemaphoreType.DMA,
            pltpu.SemaphoreType.DMA,
        ],
        name="pack",
    )(row_map, anc_order, anc_below, desc_panel)


GROUP = 4


def diag_kernel(codes, head_ref, out_ref):
    step = pl.program_id(0)

    @pl.when(step == 0)
    def _():
        out_ref[...] = jnp.zeros_like(out_ref)

    for g in range(GROUP):
        for t in range(2 * SLOTS):
            c = codes[step * GROUP + g, t * 3]

            @pl.when(c < CB)
            def _():
                block = head_ref[g, t * BR:(t + 1) * BR, :]
                place = (t // SLOTS) * CB + c
                out_ref[place] = out_ref[place] + nt_dot(block, block)


def diag_sums(codes, head):
    return pl.pallas_call(
        diag_kernel,
        out_shape=jax.ShapeDtypeStruct((2 * CB, BR, BR), jnp.float32),
        grid_spec=pltpu.PrefetchScalarGridSpec(
            num_scalar_prefetch=1,
            grid=(PLANE // GROUP,),
            in_specs=[pl.BlockSpec((GROUP, HEAD_ROWS, BR), lambda k, codes: (k, 0, 0))],
            out_specs=pl.BlockSpec((2 * CB, BR, BR), lambda k, codes: (0, 0, 0)),
        ),
        name="diag_sums",
    )(codes, head)


def below_kernel(i, codes, head_ref, tail_ref, out_ref):
    step = pl.program_id(0)

    @pl.when(step == 0)
    def _():
        out_ref[...] = jnp.zeros_like(out_ref)

    for g in range(GROUP):
        for s in range(SLOTS):
            t = i * SLOTS + s
            c = codes[step * GROUP + g, t * 3]

            @pl.when(c < CB)
            def _():
                product = nt_dot(tail_ref[g, s], head_ref[g, s * BR:(s + 1) * BR, :])
                for r in range(2):
                    j = codes[step * GROUP + g, t * 3 + 1 + r]
                    place = (((j % Y) * 2 + c // 2) * (Q // Y) + j // Y) * 2 + c % 2
                    out_ref[place] = out_ref[place] + product[r * BR:(r + 1) * BR]


def below_sums(i, codes, head, tail):
    return pl.pallas_call(
        functools.partial(below_kernel, i),
        out_shape=jax.ShapeDtypeStruct((BELOW, BR, BR), jnp.float32),
        grid_spec=pltpu.PrefetchScalarGridSpec(
            num_scalar_prefetch=1,
            grid=(PLANE // GROUP,),
            in_specs=[
                pl.BlockSpec((GROUP, SLOTS * BR, BR), lambda k, codes: (k, i, 0)),
                pl.BlockSpec((GROUP, SLOTS, 2 * BR, BR), lambda k, codes: (k, 0, 0, 0)),
            ],
            out_specs=pl.BlockSpec((BELOW, BR, BR), lambda k, codes: (0, 0, 0)),
        ),
        name=f"below_sums{i}",
    )(codes, head, tail)


def device(z, xc, y):
    return (z * XC + xc) * Y + y


def owner_z(i, xc, y):
    return y + Y * (i ^ (xc % 2))


def diag_route():
    pairs = []
    for xc in range(XC):
        for y in range(Y):
            for i in range(2):
                for c in range(CB):
                    pairs.append((device(i * CB + c, xc, y), device(owner_z(i, xc, y), xc, c)))
    return pairs


def below_route(i, h):
    pairs = []
    for xc in range(XC):
        for y in range(Y):
            for b in range(Y):
                pairs.append((device(2 * b + h, xc, y), device(owner_z(i, xc, y), xc, b)))
    return pairs


def solve_kernel(rows_ref, lower_ref, inverse_ref, u00, u01, u10, u11, out_ref):
    m = pl.program_id(0)

    @pl.when(m == 0)
    def _():
        out_ref[0, 0, 0] = lower_ref[0]

    @pl.when(m > 0)
    def _():
        first = u00[0] + u10[0]
        second = u01[0] + u11[0]
        update = jnp.concatenate([first[0], first[1], second[0], second[1]], axis=1)
        out_ref[0, 0, 0] = nt_dot(rows_ref[0, 0, 0] - update, inverse_ref[...], HIGHEST)


def solve(anc_panel, lower_strips, inverse, parts, y):
    width = anc_panel.shape[4]
    parts = [part.reshape(Q // Y, 2, BR, BR) for part in parts]
    update_spec = pl.BlockSpec((1, 2, BR, BR), lambda m, y: (jnp.maximum(m - 1, 0), 0, 0, 0))

    def kernel(y_ref, *refs):
        solve_kernel(*refs)

    return pl.pallas_call(
        kernel,
        out_shape=jax.ShapeDtypeStruct(anc_panel.shape, jnp.float32),
        grid_spec=pltpu.PrefetchScalarGridSpec(
            num_scalar_prefetch=1,
            grid=(anc_panel.shape[1],),
            in_specs=[
                pl.BlockSpec((1, 1, 1, BR, width), lambda m, y: (0, m, 0, 0, 0)),
                pl.BlockSpec((1, BR, width), lambda m, y: (y[0], 0, 0)),
                pl.BlockSpec((width, width), lambda m, y: (0, 0)),
            ] + [update_spec] * 4,
            out_specs=pl.BlockSpec((1, 1, 1, BR, width), lambda m, y: (0, m, 0, 0, 0)),
        ),
        name="solve",
    )(y, anc_panel, lower_strips, inverse, *parts)


def exchange(value):
    return lax.all_to_all(value, ("xc", "y"), split_axis=0, concat_axis=0, tiled=True)


def shards(desc_panel, row_map, anc_order, anc_below, anc_panel):
    width = anc_panel.shape[4]
    y = lax.axis_index("y")
    head, tail0, tail1 = pack(row_map, anc_order, anc_below, desc_panel)
    head = exchange(head)
    tail0, head = lax.optimization_barrier((tail0, head))
    tail0 = exchange(tail0)
    tail1, tail0 = lax.optimization_barrier((tail1, tail0))
    tail1 = exchange(tail1)
    codes = head[:, 2 * SLOTS * BR, : 2 * SLOTS * 3].astype(jnp.int32)

    diag = lax.psum_scatter(diag_sums(codes, head), "z", scatter_dimension=0, tiled=True)
    diag = lax.ppermute(diag, ALL, diag_route())
    strip = anc_panel[0, 0, 0].reshape(BR, CB, BR)
    own = (jnp.arange(CB) == y)[None, :, None]
    strip = strip - jnp.where(own, diag[0][:, None, :], 0.0)
    schur = lax.all_gather(strip.reshape(BR, width), "y", axis=0, tiled=True)
    lower = jnp.linalg.cholesky(schur, symmetrize_input=False)
    inverse = jax.scipy.linalg.solve_triangular(lower, jnp.eye(width, dtype=jnp.float32), lower=True)

    parts = []
    for i, tail in enumerate((tail0, tail1)):
        sums = lax.psum_scatter(
            below_sums(i, codes, head, tail), "z", scatter_dimension=0, tiled=True
        )
        parts += [lax.ppermute(sums, ALL, below_route(i, h)) for h in range(2)]
    return solve(anc_panel, lower.reshape(CB, BR, width), inverse, parts, y.reshape(1))


def solution(mesh):
    grid = Mesh(mesh.devices.reshape(Z, XC, Y), ALL)
    in_specs = (
        P(ALL, None, None),
        P(ALL, None),
        P(),
        P(),
        P(("z", "xc"), None, "y", None, None),
    )
    out_specs = P(("z", "xc"), None, "y", None, None)
    return jax.shard_map(shards, mesh=grid, in_specs=in_specs, out_specs=out_specs, check_vma=False)
```

```python
import functools

import jax
import jax.numpy as jnp
from jax import lax
from jax.experimental import pallas as pl
from jax.experimental.pallas import tpu as pltpu
from jax.sharding import Mesh
from jax.sharding import PartitionSpec as P

Z, XC, Y = 8, 8, 4
PLANE = XC * Y
BR = 128
CB = 4
Q = 12
SLOTS = 2
NA = 64
NONE = 7
META = 16
HEAD_ROWS = 2 * SLOTS * BR + META
BELOW = Q * CB
HIGHEST = lax.Precision.HIGHEST
NB = 16
PIECE = 2
PIECES = BELOW // PIECE
ALL = ("z", "xc", "y")


def nt_dot(a, b, precision=None):
    return lax.dot_general(
        a, b, (((1,), (1,)), ((), ())), precision=precision, preferred_element_type=jnp.float32
    )


def pack_kernel(
    map_ref, order_ref, below_ref, desc_ref, head_ref, tail0_ref, tail1_ref,
    stage, meta, inverse, used, codes, in_sems, head_sem, tail_sem, meta_sem,
):
    count = map_ref.shape[0]
    parts = in_sems.shape[0]
    step = count // parts

    def load(k):
        part = pl.ds(k * step, step)
        return pltpu.make_async_copy(desc_ref.at[part], stage.at[part], in_sems.at[k])

    for k in range(parts):
        load(k).start()

    def clear(a, carry):
        inverse[order_ref[a]] = a
        used[a] = 0
        for s in range(SLOTS):
            codes[(a * SLOTS + s) * 4] = NONE
            codes[(a * SLOTS + s) * 4 + 1] = 0
            codes[(a * SLOTS + s) * 4 + 2] = 0
        return carry

    lax.fori_loop(0, NA, clear, 0)

    def route(d, carry):
        head = map_ref[d, 0]
        a = inverse[head // CB]
        s = used[a]
        used[a] = s + 1
        dest = (a % XC) * Y + (a // XC) % Y
        i = jnp.bitwise_xor(a // (XC * Y), a % 2)
        slot = (dest * 2 + i) * SLOTS + s
        first, second = map_ref[d, 1], map_ref[d, 2]
        j1, j2 = jnp.int32(0), jnp.int32(0)
        for j in range(Q):
            g = below_ref[a, j]
            j1 = jnp.where(g == first, j, j1)
            j2 = jnp.where(g == second, j, j2)
        codes[slot * 4] = head % CB
        codes[slot * 4 + 1] = j1
        codes[slot * 4 + 2] = j2
        codes[NA * SLOTS * 4 + d] = slot
        return carry

    lax.fori_loop(0, count, route, 0)

    lane = lax.broadcasted_iota(jnp.int32, (META, 128), 1)

    def describe(dest, carry):
        row = jnp.zeros((META, 128), jnp.int32)
        for t in range(2 * SLOTS):
            for f in range(3):
                row = jnp.where(lane == t * 3 + f, codes[(dest * 2 * SLOTS + t) * 4 + f], row)
        meta[dest] = row.astype(jnp.float32).astype(jnp.bfloat16)
        return carry

    lax.fori_loop(0, PLANE, describe, 0)

    for k in range(parts):
        load(k).wait()

    def send_head(d, carry):
        slot = codes[NA * SLOTS * 4 + d]
        place = pl.multiple_of((slot % (2 * SLOTS)) * BR, BR)
        pltpu.make_async_copy(
            stage.at[d, pl.ds(0, BR)],
            head_ref.at[slot // (2 * SLOTS), pl.ds(place, BR)],
            head_sem,
        ).start()
        return carry

    lax.fori_loop(0, count, send_head, 0)
    pltpu.make_async_copy(meta, head_ref.at[:, pl.ds(2 * SLOTS * BR, META)], meta_sem).start()

    def send_tail(d, carry):
        slot = codes[NA * SLOTS * 4 + d]
        dest, i, s = slot // (2 * SLOTS), (slot // SLOTS) % 2, slot % SLOTS
        for k, out in ((0, tail0_ref), (1, tail1_ref)):
            @pl.when(i == k)
            def _():
                pltpu.make_async_copy(
                    stage.at[d, pl.ds(BR, 2 * BR)], out.at[dest, s], tail_sem
                ).start()
        return carry

    lax.fori_loop(0, count, send_tail, 0)
    pltpu.make_async_copy(meta, head_ref.at[:, pl.ds(2 * SLOTS * BR, META)], meta_sem).wait()
    heads = stage.at[:, pl.ds(0, BR)]
    pltpu.make_async_copy(heads, heads, head_sem).wait()
    tails = stage.at[:, pl.ds(BR, 2 * BR)]
    pltpu.make_async_copy(tails, tails, tail_sem).wait()


def pack(row_map, anc_order, anc_below, desc_panel):
    count = row_map.shape[0]
    smem = pl.BlockSpec(memory_space=pltpu.SMEM)
    hbm = pl.BlockSpec(memory_space=pltpu.HBM)
    dt = desc_panel.dtype
    return pl.pallas_call(
        pack_kernel,
        out_shape=(
            jax.ShapeDtypeStruct((PLANE, HEAD_ROWS, BR), dt),
            jax.ShapeDtypeStruct((PLANE, SLOTS, 2 * BR, BR), dt),
            jax.ShapeDtypeStruct((PLANE, SLOTS, 2 * BR, BR), dt),
        ),
        in_specs=[smem, smem, smem, hbm],
        out_specs=(hbm, hbm, hbm),
        scratch_shapes=[
            pltpu.VMEM(desc_panel.shape, dt),
            pltpu.VMEM((PLANE, META, BR), dt),
            pltpu.SMEM((NA,), jnp.int32),
            pltpu.SMEM((NA,), jnp.int32),
            pltpu.SMEM((NA * SLOTS * 4 + count,), jnp.int32),
            pltpu.SemaphoreType.DMA((4,)),
            pltpu.SemaphoreType.DMA,
            pltpu.SemaphoreType.DMA,
            pltpu.SemaphoreType.DMA,
        ],
        name="pack",
    )(row_map, anc_order, anc_below, desc_panel)


GROUP = 4


def diag_kernel(codes, head_ref, out_ref):
    step = pl.program_id(0)

    @pl.when(step == 0)
    def _():
        out_ref[...] = jnp.zeros_like(out_ref)

    for g in range(GROUP):
        for t in range(2 * SLOTS):
            c = codes[step * GROUP + g, t * 3]

            @pl.when(c < CB)
            def _():
                block = head_ref[g, t * BR:(t + 1) * BR, :]
                place = (t // SLOTS) * CB + c
                out_ref[place] = out_ref[place] + nt_dot(block, block)


def diag_sums(codes, head):
    return pl.pallas_call(
        diag_kernel,
        out_shape=jax.ShapeDtypeStruct((2 * CB, BR, BR), jnp.float32),
        grid_spec=pltpu.PrefetchScalarGridSpec(
            num_scalar_prefetch=1,
            grid=(PLANE // GROUP,),
            in_specs=[pl.BlockSpec((GROUP, HEAD_ROWS, BR), lambda k, codes: (k, 0, 0))],
            out_specs=pl.BlockSpec((2 * CB, BR, BR), lambda k, codes: (0, 0, 0)),
        ),
        name="diag_sums",
    )(codes, head)


def below_kernel(i, codes, head_ref, tail_ref, out_ref):
    step = pl.program_id(0)

    @pl.when(step == 0)
    def _():
        out_ref[...] = jnp.zeros_like(out_ref)

    for g in range(GROUP):
        for s in range(SLOTS):
            t = i * SLOTS + s
            c = codes[step * GROUP + g, t * 3]

            @pl.when(c < CB)
            def _():
                product = nt_dot(tail_ref[g, s], head_ref[g, s * BR:(s + 1) * BR, :])
                for r in range(2):
                    j = codes[step * GROUP + g, t * 3 + 1 + r]
                    place = ((j % Y) * (Q // Y) + j // Y) * CB + c
                    out_ref[place] = out_ref[place] + product[r * BR:(r + 1) * BR]


def below_sums(i, codes, head, tail):
    return pl.pallas_call(
        functools.partial(below_kernel, i),
        out_shape=jax.ShapeDtypeStruct((BELOW, BR, BR), jnp.float32),
        grid_spec=pltpu.PrefetchScalarGridSpec(
            num_scalar_prefetch=1,
            grid=(PLANE // GROUP,),
            in_specs=[
                pl.BlockSpec((GROUP, SLOTS * BR, BR), lambda k, codes: (k, i, 0)),
                pl.BlockSpec((GROUP, SLOTS, 2 * BR, BR), lambda k, codes: (k, 0, 0, 0)),
            ],
            out_specs=pl.BlockSpec((BELOW, BR, BR), lambda k, codes: (0, 0, 0)),
        ),
        name=f"below_sums{i}",
    )(codes, head, tail)


def nn_dot(a, b):
    return lax.dot_general(
        a, b, (((1,), (0,)), ((), ())), precision=HIGHEST, preferred_element_type=jnp.float32
    )


def tn_dot(a, b):
    return lax.dot_general(
        a, b, (((0,), (0,)), ((), ())), precision=HIGHEST, preferred_element_type=jnp.float32
    )


def factor_block(pair):
    sub = lax.broadcasted_iota(jnp.int32, (NB, BR), 0)
    sub2 = lax.broadcasted_iota(jnp.int32, (NB, 2 * BR), 0)
    lane = lax.broadcasted_iota(jnp.int32, (NB, BR), 1)
    for k in range(BR // NB):
        rows = pair[k * NB:(k + 1) * NB, :]
        cols = [jnp.broadcast_to(rows[:, k * NB + j:k * NB + j + 1], (NB, BR)) for j in range(NB)]
        for j in range(NB):
            scale = lax.rsqrt(cols[j][j:j + 1, :])
            column = cols[j] * scale
            below = jnp.where(sub > j, column, 0.0)
            row = rows[j:j + 1, :] * jnp.concatenate([scale, scale], axis=1)
            rows = jnp.where(sub2 == j, row, rows - jnp.concatenate([below, below], axis=1) * row)
            for m in range(j + 1, NB):
                cols[m] = cols[m] - below * column[m:m + 1, :]
        pair[k * NB:(k + 1) * NB, :] = rows
        start = (k + 1) * NB
        if start < BR:
            left = jnp.where(lane >= start, rows[:, :BR], 0.0)
            pair[start:, :] = pair[start:, :] - tn_dot(left, rows)[start:]


def factor_kernel(s_ref, lower_ref, inverse_ref, work, pair):
    width = s_ref.shape[0]
    work[...] = s_ref[...]
    inverse_ref[...] = jnp.zeros_like(inverse_ref)
    row = lax.broadcasted_iota(jnp.int32, (BR, BR), 0)
    col = lax.broadcasted_iota(jnp.int32, (BR, BR), 1)
    all_rows = lax.broadcasted_iota(jnp.int32, (width, BR), 0)
    wide = lax.broadcasted_iota(jnp.int32, (BR, width), 1)
    high = lax.broadcasted_iota(jnp.int32, (BR, width), 0)

    def step(kb, carry):
        at = pl.ds(pl.multiple_of(kb * BR, BR), BR)
        pair[:, :BR] = work[at, at]
        pair[:, BR:] = jnp.where(row == col, 1.0, 0.0)
        factor_block(pair)
        diagonal = jnp.where(col >= row, pair[:, :BR], 0.0).T
        small = jnp.where(col <= row, pair[:, BR:], 0.0)
        panel = nt_dot(work[:, at], small, HIGHEST)
        panel = jnp.where(all_rows >= (kb + 1) * BR, panel, 0.0)
        lower_ref[:, at] = panel
        lower_ref[at, at] = diagonal
        work[...] = work[...] - nt_dot(panel, panel, HIGHEST)
        before = jnp.where(wide < kb * BR, lower_ref[at, :], 0.0)
        target = jnp.where(wide == high + kb * BR, 1.0, 0.0) - nn_dot(before, inverse_ref[...])
        inverse_ref[at, :] = nn_dot(small, target)
        return carry

    lax.fori_loop(0, width // BR, step, 0)


def factor(schur):
    width = schur.shape[0]
    return pl.pallas_call(
        factor_kernel,
        out_shape=(jax.ShapeDtypeStruct((width, width), jnp.float32),) * 2,
        scratch_shapes=[pltpu.VMEM((width, width), jnp.float32), pltpu.VMEM((BR, 2 * BR), jnp.float32)],
        name="factor",
    )(schur)


def remote(src, dst, send_sem, recv_sem, **device):
    return pltpu.make_async_remote_copy(
        src_ref=src, dst_ref=dst, send_sem=send_sem, recv_sem=recv_sem,
        device_id=device, device_id_type=pl.DeviceIdType.MESH,
    )


def signal(semaphore, **device):
    pl.semaphore_signal(
        semaphore, inc=1, device_id=device, device_id_type=pl.DeviceIdType.MESH
    )


def target_z(i, core, y):
    return y + Y * jnp.bitwise_xor(core, i)


def diag_exchange_kernel(
    sums, strip, out, arrived, strips, blocks, mine,
    send_sems, recv_sems, strip_send, strip_recv, block_send, block_recv,
):
    z, y = lax.axis_index("z"), lax.axis_index("y")
    core = lax.axis_index("xc") % 2
    gather_y = z % Y
    here = gather_y == y

    barrier = pltpu.get_barrier_semaphore()
    for k in range(1, Y):
        signal(barrier, y=(y + k) % Y)
    for source in range(Z):
        @pl.when(jnp.logical_not(jnp.logical_and(here, source == z)))
        def _():
            signal(barrier, z=jnp.int32(source), y=gather_y)
    pl.semaphore_wait(barrier, Y - 1 + Z - here.astype(jnp.int32))

    for i in range(2):
        for c in range(CB):
            owner = target_z(i, core, y)
            local = jnp.logical_and(owner == z, c == y)

            @pl.when(jnp.logical_not(local))
            def _():
                remote(
                    sums.at[i * CB + c], arrived.at[z], send_sems.at[i * CB + c], recv_sems.at[z],
                    z=owner, y=jnp.int32(c),
                ).start()

            @pl.when(local)
            def _():
                arrived[z] = sums[i * CB + c]

    for k in range(1, Y):
        remote(
            strip.at[0, 0, 0], strips.at[y], strip_send.at[k], strip_recv.at[y], y=(y + k) % Y
        ).start()
    strips[y] = strip[0, 0, 0]

    for source in range(Z):
        @pl.when(jnp.logical_not(jnp.logical_and(here, source == z)))
        def _():
            remote(
                sums.at[0], arrived.at[source], send_sems.at[0], recv_sems.at[source], y=(y + 1) % Y
            ).wait_recv()

    update = arrived[0]
    for source in range(1, Z):
        update = update + arrived[source]
    columns = pl.ds(pl.multiple_of(y * BR, BR), BR)
    block = strip[0, 0, 0, :, columns] - update
    mine[...] = block
    blocks[y] = block
    for k in range(1, Y):
        remote(mine, blocks.at[y], block_send.at[k], block_recv.at[y], y=(y + k) % Y).start()

    for k in range(1, Y):
        other = (y + k) % Y
        remote(
            strip.at[0, 0, 0], strips.at[other], strip_send.at[k], strip_recv.at[other], y=other
        ).wait_recv()
    for k in range(Y):
        out[k * BR:(k + 1) * BR, :] = strips[k]
    for k in range(1, Y):
        other = (y + k) % Y
        remote(mine, blocks.at[other], block_send.at[k], block_recv.at[other], y=other).wait_recv()
    for k in range(Y):
        out[k * BR:(k + 1) * BR, k * BR:(k + 1) * BR] = blocks[k]

    for i in range(2):
        for c in range(CB):
            owner = target_z(i, core, y)

            @pl.when(jnp.logical_not(jnp.logical_and(owner == z, c == y)))
            def _():
                remote(
                    sums.at[i * CB + c], arrived.at[z], send_sems.at[i * CB + c], recv_sems.at[z],
                    z=owner, y=jnp.int32(c),
                ).wait_send()
    for k in range(1, Y):
        other = (y + k) % Y
        remote(
            strip.at[0, 0, 0], strips.at[y], strip_send.at[k], strip_recv.at[y], y=other
        ).wait_send()
        remote(mine, blocks.at[y], block_send.at[k], block_recv.at[y], y=other).wait_send()


def diag_exchange(sums, anc_panel):
    width = anc_panel.shape[4]
    return pl.pallas_call(
        diag_exchange_kernel,
        out_shape=jax.ShapeDtypeStruct((width, width), jnp.float32),
        grid=(1,),
        in_specs=[
            pl.BlockSpec((2 * CB, BR, BR), lambda k: (0, 0, 0)),
            pl.BlockSpec((1, 1, 1, BR, width), lambda k: (0, 0, 0, 0, 0)),
        ],
        out_specs=pl.BlockSpec((width, width), lambda k: (0, 0)),
        scratch_shapes=[
            pltpu.VMEM((Z, BR, BR), jnp.float32),
            pltpu.VMEM((Y, BR, width), jnp.float32),
            pltpu.VMEM((Y, BR, BR), jnp.float32),
            pltpu.VMEM((BR, BR), jnp.float32),
            pltpu.SemaphoreType.DMA((2 * CB,)),
            pltpu.SemaphoreType.DMA((Z,)),
            pltpu.SemaphoreType.DMA((Y,)),
            pltpu.SemaphoreType.DMA((Y,)),
            pltpu.SemaphoreType.DMA((Y,)),
            pltpu.SemaphoreType.DMA((Y,)),
        ],
        compiler_params=pltpu.CompilerParams(collective_id=0, has_side_effects=True),
        name="diag_exchange",
    )(sums, anc_panel)


def reduce_kernel(
    i, sums, out, up, down, final, up_sems, down_sems, final_sems, send_sem,
):
    z, y = lax.axis_index("z"), lax.axis_index("y")
    core = lax.axis_index("xc") % 2
    half = jnp.bitwise_xor(core, i)
    distance = (y + Y * half - z + Z) % Z
    above, under = (z + 1) % Z, (z + Z - 1) % Z
    own = PIECES // Y

    barrier = pltpu.get_barrier_semaphore()
    signal(barrier, z=above)
    signal(barrier, z=under)
    for k in range(1, Y):
        signal(barrier, y=(y + k) % Y)
    pl.semaphore_wait(barrier, Y + 1)

    def take(buffer, sems, q):
        remote(sums.at[q], buffer.at[q], send_sem, sems.at[q], z=above).wait_recv()

    def relay(buffer, sems, to):
        def body(q, carry):
            take(buffer, sems, q)
            buffer[q] = buffer[q] + sums[q]
            remote(buffer.at[q], buffer.at[q], send_sem, sems.at[q], z=to).start()
            return carry

        lax.fori_loop(0, PIECES, body, 0)

    def begin(buffer, sems, to):
        def body(q, carry):
            remote(sums.at[q], buffer.at[q], send_sem, sems.at[q], z=to).start()
            return carry

        lax.fori_loop(0, PIECES, body, 0)

    @pl.when(distance == 4)
    def _():
        begin(up, up_sems, above)

    @pl.when(distance == 5)
    def _():
        begin(down, down_sems, under)

    @pl.when(jnp.logical_and(distance >= 1, distance <= 3))
    def _():
        relay(up, up_sems, above)

    @pl.when(distance >= 6)
    def _():
        relay(down, down_sems, under)

    @pl.when(distance == 0)
    def _():
        def body(q, carry):
            take(up, up_sems, q)
            take(down, down_sems, q)
            total = up[q] + down[q] + sums[q]
            to, place = q // own, q % own

            @pl.when(to == y)
            def _():
                out[place] = total

            @pl.when(to != y)
            def _():
                up[q] = total
                remote(up.at[q], final.at[place], send_sem, final_sems.at[place], y=to).start()

            return carry

        lax.fori_loop(0, PIECES, body, 0)
        sent = up.at[pl.ds(0, PIECES - own)]
        remote(sent, sent, send_sem, up_sems.at[0], z=above).wait_send()

    @pl.when(distance != 0)
    def _():
        remote(up, up, send_sem, up_sems.at[0], z=above).wait_send()

        @pl.when(z // Y == half)
        def _():
            def body(place, carry):
                remote(
                    sums.at[place], final.at[place], send_sem, final_sems.at[place], z=above
                ).wait_recv()
                out[place] = final[place]
                return carry

            lax.fori_loop(0, own, body, 0)


def below_reduce(i, sums):
    own = PIECES // Y
    shape = (PIECE, BR, BR)
    return pl.pallas_call(
        functools.partial(reduce_kernel, i),
        out_shape=jax.ShapeDtypeStruct((own, *shape), jnp.float32),
        in_specs=[pl.BlockSpec(memory_space=pltpu.VMEM)],
        out_specs=pl.BlockSpec(memory_space=pltpu.VMEM),
        scratch_shapes=[
            pltpu.VMEM((PIECES, *shape), jnp.float32),
            pltpu.VMEM((PIECES, *shape), jnp.float32),
            pltpu.VMEM((own, *shape), jnp.float32),
            pltpu.SemaphoreType.DMA((PIECES,)),
            pltpu.SemaphoreType.DMA((PIECES,)),
            pltpu.SemaphoreType.DMA((own,)),
            pltpu.SemaphoreType.DMA,
        ],
        compiler_params=pltpu.CompilerParams(collective_id=1 + i, has_side_effects=True),
        name=f"below_reduce{i}",
    )(sums.reshape(PIECES, *shape))


def solve_kernel(where_ref, rows_ref, lower_ref, inverse_ref, update0, update1, out_ref):
    m = pl.program_id(0)

    @pl.when(m == 0)
    def _():
        out_ref[0, 0, 0] = lower_ref[...]

    for i, part in enumerate((update0, update1)):
        @pl.when(jnp.logical_and(m > 0, where_ref[1] == i))
        def _():
            update = jnp.concatenate([part[0, c] for c in range(CB)], axis=1)
            out_ref[0, 0, 0] = nt_dot(rows_ref[0, 0, 0] - update, inverse_ref[...], HIGHEST)


def solve(anc_panel, lower, inverse, updates, where):
    width = anc_panel.shape[4]
    updates = [part.reshape(Q // Y, CB, BR, BR) for part in updates]
    update_spec = pl.BlockSpec((1, CB, BR, BR), lambda m, w: (jnp.maximum(m - 1, 0), 0, 0, 0))
    return pl.pallas_call(
        solve_kernel,
        out_shape=jax.ShapeDtypeStruct(anc_panel.shape, jnp.float32),
        grid_spec=pltpu.PrefetchScalarGridSpec(
            num_scalar_prefetch=1,
            grid=(anc_panel.shape[1],),
            in_specs=[
                pl.BlockSpec((1, 1, 1, BR, width), lambda m, w: (0, m, 0, 0, 0)),
                pl.BlockSpec((BR, width), lambda m, w: (w[0], 0)),
                pl.BlockSpec((width, width), lambda m, w: (0, 0)),
            ] + [update_spec] * 2,
            out_specs=pl.BlockSpec((1, 1, 1, BR, width), lambda m, w: (0, m, 0, 0, 0)),
        ),
        name="solve",
    )(where, anc_panel, lower, inverse, *updates)


def exchange(value):
    return lax.all_to_all(value, ("xc", "y"), split_axis=0, concat_axis=0, tiled=True)


def shards(desc_panel, row_map, anc_order, anc_below, anc_panel):
    z, xc, y = (lax.axis_index(axis) for axis in ALL)
    head, tail0, tail1 = pack(row_map, anc_order, anc_below, desc_panel)
    head = exchange(head)
    tail0, head = lax.optimization_barrier((tail0, head))
    tail0 = exchange(tail0)
    codes = head[:, 2 * SLOTS * BR, : 2 * SLOTS * 3].astype(jnp.int32)
    schur = diag_exchange(diag_sums(codes, head), anc_panel)
    lower, inverse = factor(schur)
    tail1, tail0, lower = lax.optimization_barrier((tail1, tail0, lower))
    tail1 = exchange(tail1)
    update0 = below_reduce(0, below_sums(0, codes, head, tail0))
    tail1, update0 = lax.optimization_barrier((tail1, update0))
    update1 = below_reduce(1, below_sums(1, codes, head, tail1))
    where = jnp.stack([y, jnp.bitwise_xor(z // Y, xc % 2)]).astype(jnp.int32)
    return solve(anc_panel, lower, inverse, (update0, update1), where)


def solution(mesh):
    grid = Mesh(mesh.devices.reshape(Z, XC, Y), ALL)
    in_specs = (
        P(ALL, None, None),
        P(ALL, None),
        P(),
        P(),
        P(("z", "xc"), None, "y", None, None),
    )
    out_specs = P(("z", "xc"), None, "y", None, None)
    return jax.shard_map(shards, mesh=grid, in_specs=in_specs, out_specs=out_specs, check_vma=False)
```

```python
import functools

import jax
import jax.numpy as jnp
from jax import lax
from jax.experimental import pallas as pl
from jax.experimental.pallas import tpu as pltpu
from jax.sharding import Mesh
from jax.sharding import PartitionSpec as P

Z, XC, Y = 8, 8, 4
PLANE = XC * Y
BR = 128
CB = 4
Q = 12
SLOTS = 2
NA = 64
NONE = 7
META = 16
HEAD_ROWS = 2 * SLOTS * BR + META
BELOW = Q * CB
HIGHEST = lax.Precision.HIGHEST
NB = 16
PIECE = 2
PIECES = BELOW // PIECE
ALL = ("z", "xc", "y")


def nt_dot(a, b, precision=None):
    return lax.dot_general(
        a, b, (((1,), (1,)), ((), ())), precision=precision, preferred_element_type=jnp.float32
    )


def pack_kernel(
    map_ref, order_ref, below_ref, desc_ref, head_ref, tail0_ref, tail1_ref,
    stage, meta, inverse, used, codes, in_sems, head_sem, tail_sem, meta_sem,
):
    count = map_ref.shape[1]
    parts = in_sems.shape[0]
    step = count // parts

    def load(k):
        part = pl.ds(k * step, step)
        return pltpu.make_async_copy(desc_ref.at[part], stage.at[part], in_sems.at[k])

    for k in range(parts):
        load(k).start()

    def clear(a, carry):
        inverse[order_ref[a]] = a
        used[a] = 0
        for s in range(SLOTS):
            codes[(a * SLOTS + s) * 4] = NONE
            codes[(a * SLOTS + s) * 4 + 1] = 0
            codes[(a * SLOTS + s) * 4 + 2] = 0
        return carry

    lax.fori_loop(0, NA, clear, 0)

    def route(d, carry):
        head = map_ref[0, d]
        a = inverse[head // CB]
        s = used[a]
        used[a] = s + 1
        dest = (a % XC) * Y + (a // XC) % Y
        i = jnp.bitwise_xor(a // (XC * Y), a % 2)
        slot = (dest * 2 + i) * SLOTS + s
        first, second = map_ref[1, d], map_ref[2, d]
        j1, j2 = jnp.int32(0), jnp.int32(0)
        for j in range(Q):
            g = below_ref[j, a]
            j1 = jnp.where(g == first, j, j1)
            j2 = jnp.where(g == second, j, j2)
        codes[slot * 4] = head % CB
        codes[slot * 4 + 1] = j1
        codes[slot * 4 + 2] = j2
        codes[NA * SLOTS * 4 + d] = slot
        return carry

    lax.fori_loop(0, count, route, 0)

    lane = lax.broadcasted_iota(jnp.int32, (META, 128), 1)

    def describe(dest, carry):
        row = jnp.zeros((META, 128), jnp.int32)
        for t in range(2 * SLOTS):
            for f in range(3):
                row = jnp.where(lane == t * 3 + f, codes[(dest * 2 * SLOTS + t) * 4 + f], row)
        meta[dest] = row.astype(jnp.float32).astype(jnp.bfloat16)
        return carry

    lax.fori_loop(0, PLANE, describe, 0)

    for k in range(parts):
        load(k).wait()

    def send_head(d, carry):
        slot = codes[NA * SLOTS * 4 + d]
        place = pl.multiple_of((slot % (2 * SLOTS)) * BR, BR)
        pltpu.make_async_copy(
            stage.at[d, pl.ds(0, BR)],
            head_ref.at[slot // (2 * SLOTS), pl.ds(place, BR)],
            head_sem,
        ).start()
        return carry

    lax.fori_loop(0, count, send_head, 0)
    pltpu.make_async_copy(meta, head_ref.at[:, pl.ds(2 * SLOTS * BR, META)], meta_sem).start()

    def send_tail(d, carry):
        slot = codes[NA * SLOTS * 4 + d]
        dest, i, s = slot // (2 * SLOTS), (slot // SLOTS) % 2, slot % SLOTS
        for k, out in ((0, tail0_ref), (1, tail1_ref)):
            @pl.when(i == k)
            def _():
                pltpu.make_async_copy(
                    stage.at[d, pl.ds(BR, 2 * BR)], out.at[dest, s], tail_sem
                ).start()
        return carry

    lax.fori_loop(0, count, send_tail, 0)
    pltpu.make_async_copy(meta, head_ref.at[:, pl.ds(2 * SLOTS * BR, META)], meta_sem).wait()
    heads = stage.at[:, pl.ds(0, BR)]
    pltpu.make_async_copy(heads, heads, head_sem).wait()
    tails = stage.at[:, pl.ds(BR, 2 * BR)]
    pltpu.make_async_copy(tails, tails, tail_sem).wait()


def pack(row_map, anc_order, anc_below, desc_panel):
    count = row_map.shape[0]
    smem = pl.BlockSpec(memory_space=pltpu.SMEM)
    hbm = pl.BlockSpec(memory_space=pltpu.HBM)
    dt = desc_panel.dtype
    return pl.pallas_call(
        pack_kernel,
        out_shape=(
            jax.ShapeDtypeStruct((PLANE, HEAD_ROWS, BR), dt),
            jax.ShapeDtypeStruct((PLANE, SLOTS, 2 * BR, BR), dt),
            jax.ShapeDtypeStruct((PLANE, SLOTS, 2 * BR, BR), dt),
        ),
        in_specs=[smem, smem, smem, hbm],
        out_specs=(hbm, hbm, hbm),
        scratch_shapes=[
            pltpu.VMEM(desc_panel.shape, dt),
            pltpu.VMEM((PLANE, META, BR), dt),
            pltpu.SMEM((NA,), jnp.int32),
            pltpu.SMEM((NA,), jnp.int32),
            pltpu.SMEM((NA * SLOTS * 4 + count,), jnp.int32),
            pltpu.SemaphoreType.DMA((4,)),
            pltpu.SemaphoreType.DMA,
            pltpu.SemaphoreType.DMA,
            pltpu.SemaphoreType.DMA,
        ],
        name="pack",
    )(row_map.T, anc_order, anc_below.T, desc_panel)


GROUP = 8


def diag_kernel(codes, head_ref, out_ref):
    step = pl.program_id(0)

    @pl.when(step == 0)
    def _():
        out_ref[...] = jnp.zeros_like(out_ref)

    for g in range(GROUP):
        blocks = [head_ref[g, t * BR:(t + 1) * BR, :] for t in range(2 * SLOTS)]
        products = [nt_dot(block, block) for block in blocks]
        for t, product in enumerate(products):
            c = codes[step * GROUP + g, t * 3]
            place = jnp.where(c < CB, (t // SLOTS) * CB + c, 2 * CB)
            out_ref[place] = out_ref[place] + product


def diag_sums(codes, head):
    return pl.pallas_call(
        diag_kernel,
        out_shape=jax.ShapeDtypeStruct((2 * CB + 1, BR, BR), jnp.float32),
        grid_spec=pltpu.PrefetchScalarGridSpec(
            num_scalar_prefetch=1,
            grid=(PLANE // GROUP,),
            in_specs=[pl.BlockSpec((GROUP, HEAD_ROWS, BR), lambda k, codes: (k, 0, 0))],
            out_specs=pl.BlockSpec((2 * CB + 1, BR, BR), lambda k, codes: (0, 0, 0)),
        ),
        name="diag_sums",
    )(codes, head)


def below_kernel(i, codes, head_ref, tail_ref, out_ref):
    step = pl.program_id(0)

    @pl.when(step == 0)
    def _():
        out_ref[...] = jnp.zeros_like(out_ref)

    for g in range(GROUP):
        products = [
            nt_dot(tail_ref[g, s], head_ref[g, s * BR:(s + 1) * BR, :]) for s in range(SLOTS)
        ]
        for s, product in enumerate(products):
            t = i * SLOTS + s
            c = codes[step * GROUP + g, t * 3]
            for r in range(2):
                j = codes[step * GROUP + g, t * 3 + 1 + r]
                place = ((j % Y) * (Q // Y) + j // Y) * CB + c
                place = jnp.where(c < CB, place, BELOW)
                out_ref[place] = out_ref[place] + product[r * BR:(r + 1) * BR]


def below_sums(i, codes, head, tail):
    return pl.pallas_call(
        functools.partial(below_kernel, i),
        out_shape=jax.ShapeDtypeStruct((BELOW + PIECE, BR, BR), jnp.float32),
        grid_spec=pltpu.PrefetchScalarGridSpec(
            num_scalar_prefetch=1,
            grid=(PLANE // GROUP,),
            in_specs=[
                pl.BlockSpec((GROUP, SLOTS * BR, BR), lambda k, codes: (k, i, 0)),
                pl.BlockSpec((GROUP, SLOTS, 2 * BR, BR), lambda k, codes: (k, 0, 0, 0)),
            ],
            out_specs=pl.BlockSpec((BELOW + PIECE, BR, BR), lambda k, codes: (0, 0, 0)),
        ),
        name=f"below_sums{i}",
    )(codes, head, tail)


def nn_dot(a, b):
    return lax.dot_general(
        a, b, (((1,), (0,)), ((), ())), precision=HIGHEST, preferred_element_type=jnp.float32
    )


def tn_dot(a, b):
    return lax.dot_general(
        a, b, (((0,), (0,)), ((), ())), precision=HIGHEST, preferred_element_type=jnp.float32
    )


def factor_block(pair, between):
    sub = lax.broadcasted_iota(jnp.int32, (NB, BR), 0)
    sub2 = lax.broadcasted_iota(jnp.int32, (NB, 2 * BR), 0)
    lane = lax.broadcasted_iota(jnp.int32, (NB, BR), 1)
    for k in range(BR // NB):
        between(k)
        rows = pair[k * NB:(k + 1) * NB, :]
        cols = [jnp.broadcast_to(rows[:, k * NB + j:k * NB + j + 1], (NB, BR)) for j in range(NB)]
        for j in range(NB):
            scale = lax.rsqrt(cols[j][j:j + 1, :])
            column = cols[j] * scale
            below = jnp.where(sub > j, column, 0.0)
            row = rows[j:j + 1, :] * jnp.concatenate([scale, scale], axis=1)
            rows = jnp.where(sub2 == j, row, rows - jnp.concatenate([below, below], axis=1) * row)
            for m in range(j + 1, NB):
                cols[m] = cols[m] - below * column[m:m + 1, :]
        pair[k * NB:(k + 1) * NB, :] = rows
        start = (k + 1) * NB
        if start < BR:
            left = jnp.where(lane >= start, rows[:, :BR], 0.0)
            pair[start:, :] = pair[start:, :] - tn_dot(left, rows)[start:]


def factor_whole(s_ref, lower_ref, inverse_ref, work, pair, between):
    width = s_ref.shape[0]
    work[...] = s_ref[...]
    inverse_ref[...] = jnp.zeros_like(inverse_ref)
    row = lax.broadcasted_iota(jnp.int32, (BR, BR), 0)
    col = lax.broadcasted_iota(jnp.int32, (BR, BR), 1)
    all_rows = lax.broadcasted_iota(jnp.int32, (width, BR), 0)
    wide = lax.broadcasted_iota(jnp.int32, (BR, width), 1)
    high = lax.broadcasted_iota(jnp.int32, (BR, width), 0)

    def step(kb, carry):
        at = pl.ds(pl.multiple_of(kb * BR, BR), BR)
        pair[:, :BR] = work[at, at]
        pair[:, BR:] = jnp.where(row == col, 1.0, 0.0)
        factor_block(pair, functools.partial(between, kb))
        diagonal = jnp.where(col >= row, pair[:, :BR], 0.0).T
        small = jnp.where(col <= row, pair[:, BR:], 0.0)
        panel = nt_dot(work[:, at], small, HIGHEST)
        panel = jnp.where(all_rows >= (kb + 1) * BR, panel, 0.0)
        lower_ref[:, at] = panel
        lower_ref[at, at] = diagonal
        work[...] = work[...] - nt_dot(panel, panel, HIGHEST)
        before = jnp.where(wide < kb * BR, lower_ref[at, :], 0.0)
        target = jnp.where(wide == high + kb * BR, 1.0, 0.0) - nn_dot(before, inverse_ref[...])
        inverse_ref[at, :] = nn_dot(small, target)
        return carry

    lax.fori_loop(0, width // BR, step, 0)


def remote(src, dst, send_sem, recv_sem, **device):
    return pltpu.make_async_remote_copy(
        src_ref=src, dst_ref=dst, send_sem=send_sem, recv_sem=recv_sem,
        device_id=device, device_id_type=pl.DeviceIdType.MESH,
    )


def signal(semaphore, **device):
    pl.semaphore_signal(
        semaphore, inc=1, device_id=device, device_id_type=pl.DeviceIdType.MESH
    )


def target_z(i, core, y):
    return y + Y * jnp.bitwise_xor(core, i)


def diag_exchange_kernel(
    sums, strip, out, arrived, ones, twos, blocks, mine,
    send_sems, recv_sems, one_send, one_recv, two_send, two_recv, block_send, block_recv,
):
    z, y = lax.axis_index("z"), lax.axis_index("y")
    core = lax.axis_index("xc") % 2
    gather_y = z % Y
    here = gather_y == y

    barrier = pltpu.get_barrier_semaphore()
    for k in range(1, Y):
        signal(barrier, y=(y + k) % Y)
    for source in range(Z):
        @pl.when(jnp.logical_not(jnp.logical_and(here, source == z)))
        def _():
            signal(barrier, z=jnp.int32(source), y=gather_y)
    pl.semaphore_wait(barrier, Y - 1 + Z - here.astype(jnp.int32))

    for i in range(2):
        for c in range(CB):
            owner = target_z(i, core, y)
            local = jnp.logical_and(owner == z, c == y)

            @pl.when(jnp.logical_not(local))
            def _():
                remote(
                    sums.at[i * CB + c], arrived.at[z], send_sems.at[i * CB + c], recv_sems.at[z],
                    z=owner, y=jnp.int32(c),
                ).start()

            @pl.when(local)
            def _():
                arrived[z] = sums[i * CB + c]

    first = pl.ds(pl.multiple_of((y + Y - 1) % Y * BR, BR), BR)
    second = pl.ds(pl.multiple_of((y + 2) % Y * BR, BR), BR)
    for k in range(1, Y):
        remote(
            strip.at[0, 0, 0, :, first], ones.at[y], one_send.at[k], one_recv.at[y], y=(y + k) % Y
        ).start()
    ones[y] = strip[0, 0, 0, :, first]

    @pl.when(y >= 2)
    def _():
        for k in range(1, Y):
            remote(
                strip.at[0, 0, 0, :, second], twos.at[y], two_send.at[k], two_recv.at[y],
                y=(y + k) % Y,
            ).start()
        twos[y] = strip[0, 0, 0, :, second]

    for source in range(Z):
        @pl.when(jnp.logical_not(jnp.logical_and(here, source == z)))
        def _():
            remote(
                sums.at[0], arrived.at[source], send_sems.at[0], recv_sems.at[source], y=(y + 1) % Y
            ).wait_recv()

    update = arrived[0]
    for source in range(1, Z):
        update = update + arrived[source]
    columns = pl.ds(pl.multiple_of(y * BR, BR), BR)
    block = strip[0, 0, 0, :, columns] - update
    mine[...] = block
    blocks[y] = block
    for k in range(1, Y):
        remote(mine, blocks.at[y], block_send.at[k], block_recv.at[y], y=(y + k) % Y).start()

    for k in range(1, Y):
        other = (y + k) % Y
        remote(
            strip.at[0, 0, 0, :, first], ones.at[other], one_send.at[k], one_recv.at[other], y=other
        ).wait_recv()

        @pl.when(other >= 2)
        def _():
            remote(
                strip.at[0, 0, 0, :, second], twos.at[other], two_send.at[k], two_recv.at[other],
                y=other,
            ).wait_recv()
    out[...] = jnp.zeros_like(out)
    lower = {(1, 0): ones[1], (2, 1): ones[2], (3, 2): ones[3], (3, 0): ones[0].T,
             (2, 0): twos[2], (3, 1): twos[3]}
    for (b, c), block in lower.items():
        out[b * BR:(b + 1) * BR, c * BR:(c + 1) * BR] = block
    for k in range(1, Y):
        other = (y + k) % Y
        remote(mine, blocks.at[other], block_send.at[k], block_recv.at[other], y=other).wait_recv()
    for k in range(Y):
        out[k * BR:(k + 1) * BR, k * BR:(k + 1) * BR] = blocks[k]

    for i in range(2):
        for c in range(CB):
            owner = target_z(i, core, y)

            @pl.when(jnp.logical_not(jnp.logical_and(owner == z, c == y)))
            def _():
                remote(
                    sums.at[i * CB + c], arrived.at[z], send_sems.at[i * CB + c], recv_sems.at[z],
                    z=owner, y=jnp.int32(c),
                ).wait_send()
    for k in range(1, Y):
        other = (y + k) % Y
        remote(
            strip.at[0, 0, 0, :, first], ones.at[y], one_send.at[k], one_recv.at[y], y=other
        ).wait_send()
        remote(mine, blocks.at[y], block_send.at[k], block_recv.at[y], y=other).wait_send()

        @pl.when(y >= 2)
        def _():
            remote(
                strip.at[0, 0, 0, :, second], twos.at[y], two_send.at[k], two_recv.at[y], y=other
            ).wait_send()


def diag_exchange(sums, anc_panel):
    width = anc_panel.shape[4]
    return pl.pallas_call(
        diag_exchange_kernel,
        out_shape=jax.ShapeDtypeStruct((width, width), jnp.float32),
        grid=(1,),
        in_specs=[
            pl.BlockSpec((2 * CB + 1, BR, BR), lambda k: (0, 0, 0)),
            pl.BlockSpec((1, 1, 1, BR, width), lambda k: (0, 0, 0, 0, 0)),
        ],
        out_specs=pl.BlockSpec((width, width), lambda k: (0, 0)),
        scratch_shapes=[
            pltpu.VMEM((Z, BR, BR), jnp.float32),
            pltpu.VMEM((Y, BR, BR), jnp.float32),
            pltpu.VMEM((Y, BR, BR), jnp.float32),
            pltpu.VMEM((Y, BR, BR), jnp.float32),
            pltpu.VMEM((BR, BR), jnp.float32),
            pltpu.SemaphoreType.DMA((2 * CB,)),
            pltpu.SemaphoreType.DMA((Z,)),
            pltpu.SemaphoreType.DMA((Y,)),
            pltpu.SemaphoreType.DMA((Y,)),
            pltpu.SemaphoreType.DMA((Y,)),
            pltpu.SemaphoreType.DMA((Y,)),
            pltpu.SemaphoreType.DMA((Y,)),
            pltpu.SemaphoreType.DMA((Y,)),
        ],
        compiler_params=pltpu.CompilerParams(collective_id=0, has_side_effects=True),
        name="diag_exchange",
    )(sums, anc_panel)


class Chain:
    def __init__(self, i, sums, up, down, up_sems, down_sems, send_sem):
        self.z, self.y = lax.axis_index("z"), lax.axis_index("y")
        self.distance = (target_z(i, lax.axis_index("xc") % 2, self.y) - self.z + Z) % Z
        self.above, self.under = (self.z + 1) % Z, (self.z + Z - 1) % Z
        self.sums, self.up, self.down = sums, up, down
        self.up_sems, self.down_sems, self.send_sem = up_sems, down_sems, send_sem

    def meet(self, barrier):
        signal(barrier, z=self.above)
        signal(barrier, z=self.under)

    def copy(self, source, buffer, sems, q, to):
        return remote(source.at[q], buffer.at[q], self.send_sem, sems.at[q], z=to)

    def begin(self):
        for distance, buffer, sems, to in (
            (4, self.up, self.up_sems, self.above), (5, self.down, self.down_sems, self.under)
        ):
            @pl.when(self.distance == distance)
            def _():
                def body(q, carry):
                    self.copy(self.sums, buffer, sems, q, to).start()
                    return carry

                lax.fori_loop(0, PIECES, body, 0)

    def advance(self, q, deliver):
        for some, buffer, sems, to in (
            (jnp.logical_and(self.distance >= 1, self.distance <= 3),
             self.up, self.up_sems, self.above),
            (self.distance >= 6, self.down, self.down_sems, self.under),
        ):
            @pl.when(some)
            def _():
                self.copy(self.sums, buffer, sems, q, to).wait_recv()
                buffer[q] = buffer[q] + self.sums[q]
                self.copy(buffer, buffer, sems, q, to).start()

        @pl.when(self.distance == 0)
        def _():
            self.copy(self.sums, self.up, self.up_sems, q, self.above).wait_recv()
            self.copy(self.sums, self.down, self.down_sems, q, self.above).wait_recv()
            deliver(q, self.up[q] + self.down[q] + self.sums[q])

    def finish(self):
        @pl.when(self.distance != 0)
        def _():
            remote(self.up, self.up, self.send_sem, self.up_sems.at[0], z=self.above).wait_send()


CHAIN_SCRATCH = [
    pltpu.VMEM((PIECES, PIECE, BR, BR), jnp.float32),
    pltpu.VMEM((PIECES, PIECE, BR, BR), jnp.float32),
    pltpu.SemaphoreType.DMA((PIECES,)),
    pltpu.SemaphoreType.DMA((PIECES,)),
    pltpu.SemaphoreType.DMA,
]
IN_VMEM = pl.BlockSpec(memory_space=pltpu.VMEM)


def first_kernel(sums, schur, total, lower, inverse, up, down, up_sems, down_sems, send_sem, work, pair):
    chain = Chain(0, sums, up, down, up_sems, down_sems, send_sem)
    barrier = pltpu.get_barrier_semaphore()
    chain.meet(barrier)
    pl.semaphore_wait(barrier, 2)
    chain.begin()

    def deliver(q, value):
        total[q] = value

    each = PIECES // CB

    def between(kb, k):
        if k < each:
            chain.advance(kb * each + k, deliver)

    factor_whole(schur, lower, inverse, work, pair, between)
    chain.finish()


def first_reduce(sums, schur):
    shape = jax.ShapeDtypeStruct(schur.shape, jnp.float32)
    return pl.pallas_call(
        first_kernel,
        out_shape=(jax.ShapeDtypeStruct((PIECES, PIECE, BR, BR), jnp.float32), shape, shape),
        in_specs=[IN_VMEM] * 2,
        out_specs=(IN_VMEM,) * 3,
        scratch_shapes=CHAIN_SCRATCH + [
            pltpu.VMEM(schur.shape, jnp.float32),
            pltpu.VMEM((BR, 2 * BR), jnp.float32),
        ],
        compiler_params=pltpu.CompilerParams(collective_id=1, has_side_effects=True),
        name="first_reduce",
    )(sums.reshape(PIECES + 1, PIECE, BR, BR), schur)


def second_kernel(
    sums, total, out, up, down, up_sems, down_sems, send_sem, final, final_sems, spread_sem
):
    chain = Chain(1, sums, up, down, up_sems, down_sems, send_sem)
    z, y = chain.z, chain.y
    has_first = chain.distance == 4
    own = PIECES // Y
    barrier = pltpu.get_barrier_semaphore()
    chain.meet(barrier)
    for k in range(1, Y):
        signal(barrier, y=(y + k) % Y)
    pl.semaphore_wait(barrier, Y + 1)
    chain.begin()

    def spread(source, q):
        return remote(source.at[q], final.at[q % own], spread_sem, final_sems.at[q % own], y=q // own)

    @pl.when(has_first)
    def _():
        def body(q, carry):
            @pl.when(q // own == y)
            def _():
                out[q % own] = total[q]

            @pl.when(q // own != y)
            def _():
                spread(total, q).start()

            return carry

        lax.fori_loop(0, PIECES, body, 0)

    def deliver(q, value):
        @pl.when(q // own == y)
        def _():
            out[q % own] = value

        @pl.when(q // own != y)
        def _():
            up[q] = value
            spread(up, q).start()

    def body(q, carry):
        chain.advance(q, deliver)
        return carry

    lax.fori_loop(0, PIECES, body, 0)
    chain.finish()

    @pl.when(z % Y == y)
    def _():
        part = up.at[pl.ds(0, PIECES - own)]
        remote(part, part, spread_sem, up_sems.at[0], z=chain.above).wait_send()

    @pl.when(z % Y != y)
    def _():
        def body(place, carry):
            chain.copy(sums, final, final_sems, place, chain.above).wait_recv()
            out[place] = final[place]
            return carry

        lax.fori_loop(0, own, body, 0)


def second_reduce(sums, total):
    own = PIECES // Y
    return pl.pallas_call(
        second_kernel,
        out_shape=jax.ShapeDtypeStruct((own, PIECE, BR, BR), jnp.float32),
        in_specs=[IN_VMEM] * 2,
        out_specs=IN_VMEM,
        scratch_shapes=CHAIN_SCRATCH + [
            pltpu.VMEM((own, PIECE, BR, BR), jnp.float32),
            pltpu.SemaphoreType.DMA((own,)),
            pltpu.SemaphoreType.DMA,
        ],
        compiler_params=pltpu.CompilerParams(collective_id=2, has_side_effects=True),
        name="second_reduce",
    )(sums.reshape(PIECES + 1, PIECE, BR, BR), total)


def solve_kernel(y_ref, rows_ref, lower_ref, inverse_ref, update_ref, out_ref):
    m = pl.program_id(0)

    @pl.when(m == 0)
    def _():
        out_ref[0, 0, 0] = lower_ref[...]

    @pl.when(m > 0)
    def _():
        update = jnp.concatenate([update_ref[0, c] for c in range(CB)], axis=1)
        out_ref[0, 0, 0] = nt_dot(rows_ref[0, 0, 0] - update, inverse_ref[...], HIGHEST)


def solve(anc_panel, lower, inverse, update, y):
    width = anc_panel.shape[4]
    update = update.reshape(Q // Y, CB, BR, BR)
    return pl.pallas_call(
        solve_kernel,
        out_shape=jax.ShapeDtypeStruct(anc_panel.shape, jnp.float32),
        grid_spec=pltpu.PrefetchScalarGridSpec(
            num_scalar_prefetch=1,
            grid=(anc_panel.shape[1],),
            in_specs=[
                pl.BlockSpec((1, 1, 1, BR, width), lambda m, y: (0, m, 0, 0, 0)),
                pl.BlockSpec((BR, width), lambda m, y: (y[0], 0)),
                pl.BlockSpec((width, width), lambda m, y: (0, 0)),
                pl.BlockSpec((1, CB, BR, BR), lambda m, y: (jnp.maximum(m - 1, 0), 0, 0, 0)),
            ],
            out_specs=pl.BlockSpec((1, 1, 1, BR, width), lambda m, y: (0, m, 0, 0, 0)),
        ),
        name="solve",
    )(y, anc_panel, lower, inverse, update)


def exchange(value):
    return lax.all_to_all(value, ("xc", "y"), split_axis=0, concat_axis=0, tiled=True)


def shards(desc_panel, row_map, anc_order, anc_below, anc_panel):
    y = lax.axis_index("y").astype(jnp.int32).reshape(1)
    head, tail0, tail1 = pack(row_map, anc_order, anc_below, desc_panel)
    head = exchange(head)
    tail0, head = lax.optimization_barrier((tail0, head))
    tail0 = exchange(tail0)
    codes = head[:, 2 * SLOTS * BR, : 2 * SLOTS * 3].astype(jnp.int32)
    schur = diag_exchange(diag_sums(codes, head), anc_panel)
    tail1, tail0, schur = lax.optimization_barrier((tail1, tail0, schur))
    tail1 = exchange(tail1)
    total, lower, inverse = first_reduce(below_sums(0, codes, head, tail0), schur)
    tail1, total = lax.optimization_barrier((tail1, total))
    update = second_reduce(below_sums(1, codes, head, tail1), total)
    return solve(anc_panel, lower, inverse, update, y)


def solution(mesh):
    grid = Mesh(mesh.devices.reshape(Z, XC, Y), ALL)
    in_specs = (
        P(ALL, None, None),
        P(ALL, None),
        P(),
        P(),
        P(("z", "xc"), None, "y", None, None),
    )
    out_specs = P(("z", "xc"), None, "y", None, None)
    return jax.shard_map(shards, mesh=grid, in_specs=in_specs, out_specs=out_specs, check_vma=False)
```

```python
import functools

import jax
import jax.numpy as jnp
from jax import lax
from jax.experimental import pallas as pl
from jax.experimental.pallas import tpu as pltpu
from jax.sharding import Mesh
from jax.sharding import PartitionSpec as P

Z, XC, Y = 8, 8, 4
PLANE = XC * Y
BR = 128
CB = 4
Q = 12
SLOTS = 2
NA = 64
NONE = 7
META = 16
HEAD_ROWS = 2 * SLOTS * BR + META
BELOW = Q * CB
HIGHEST = lax.Precision.HIGHEST
NB = 16
PIECE = 2
PIECES = BELOW // PIECE
ALL = ("z", "xc", "y")


def nt_dot(a, b, precision=None):
    return lax.dot_general(
        a, b, (((1,), (1,)), ((), ())), precision=precision, preferred_element_type=jnp.float32
    )


def pack_kernel(
    map_ref, order_ref, below_ref, desc_ref, head_ref, tail0_ref, tail1_ref,
    stage, meta, inverse, used, codes, in_sems, head_sem, tail_sem, meta_sem,
):
    count = map_ref.shape[1]
    parts = in_sems.shape[0]
    step = count // parts

    def load(k):
        part = pl.ds(k * step, step)
        return pltpu.make_async_copy(desc_ref.at[part], stage.at[part], in_sems.at[k])

    for k in range(parts):
        load(k).start()

    def clear(a, carry):
        inverse[order_ref[a]] = a
        used[a] = 0
        for s in range(SLOTS):
            codes[(a * SLOTS + s) * 4] = NONE
            codes[(a * SLOTS + s) * 4 + 1] = 0
            codes[(a * SLOTS + s) * 4 + 2] = 0
        return carry

    lax.fori_loop(0, NA, clear, 0)

    def route(d, carry):
        head = map_ref[0, d]
        a = inverse[head // CB]
        s = used[a]
        used[a] = s + 1
        dest = (a % XC) * Y + (a // XC) % Y
        i = jnp.bitwise_xor(a // (XC * Y), a % 2)
        slot = (dest * 2 + i) * SLOTS + s
        first, second = map_ref[1, d], map_ref[2, d]
        j1, j2 = jnp.int32(0), jnp.int32(0)
        for j in range(Q):
            g = below_ref[j, a]
            j1 = jnp.where(g == first, j, j1)
            j2 = jnp.where(g == second, j, j2)
        codes[slot * 4] = head % CB
        codes[slot * 4 + 1] = j1
        codes[slot * 4 + 2] = j2
        codes[NA * SLOTS * 4 + d] = slot
        return carry

    lax.fori_loop(0, count, route, 0)

    lane = lax.broadcasted_iota(jnp.int32, (META, 128), 1)

    def describe(dest, carry):
        row = jnp.zeros((META, 128), jnp.int32)
        for t in range(2 * SLOTS):
            for f in range(3):
                row = jnp.where(lane == t * 3 + f, codes[(dest * 2 * SLOTS + t) * 4 + f], row)
        meta[dest] = row.astype(jnp.float32).astype(jnp.bfloat16)
        return carry

    lax.fori_loop(0, PLANE, describe, 0)

    for k in range(parts):
        load(k).wait()

    def send_head(d, carry):
        slot = codes[NA * SLOTS * 4 + d]
        place = pl.multiple_of((slot % (2 * SLOTS)) * BR, BR)
        pltpu.make_async_copy(
            stage.at[d, pl.ds(0, BR)],
            head_ref.at[slot // (2 * SLOTS), pl.ds(place, BR)],
            head_sem,
        ).start()
        return carry

    lax.fori_loop(0, count, send_head, 0)
    pltpu.make_async_copy(meta, head_ref.at[:, pl.ds(2 * SLOTS * BR, META)], meta_sem).start()

    def send_tail(d, carry):
        slot = codes[NA * SLOTS * 4 + d]
        dest, i, s = slot // (2 * SLOTS), (slot // SLOTS) % 2, slot % SLOTS
        for k, out in ((0, tail0_ref), (1, tail1_ref)):
            @pl.when(i == k)
            def _():
                pltpu.make_async_copy(
                    stage.at[d, pl.ds(BR, 2 * BR)], out.at[dest, s], tail_sem
                ).start()
        return carry

    lax.fori_loop(0, count, send_tail, 0)
    pltpu.make_async_copy(meta, head_ref.at[:, pl.ds(2 * SLOTS * BR, META)], meta_sem).wait()
    heads = stage.at[:, pl.ds(0, BR)]
    pltpu.make_async_copy(heads, heads, head_sem).wait()
    tails = stage.at[:, pl.ds(BR, 2 * BR)]
    pltpu.make_async_copy(tails, tails, tail_sem).wait()


def pack(row_map, anc_order, anc_below, desc_panel):
    count = row_map.shape[0]
    smem = pl.BlockSpec(memory_space=pltpu.SMEM)
    hbm = pl.BlockSpec(memory_space=pltpu.HBM)
    dt = desc_panel.dtype
    return pl.pallas_call(
        pack_kernel,
        out_shape=(
            jax.ShapeDtypeStruct((PLANE, HEAD_ROWS, BR), dt),
            jax.ShapeDtypeStruct((PLANE, SLOTS, 2 * BR, BR), dt),
            jax.ShapeDtypeStruct((PLANE, SLOTS, 2 * BR, BR), dt),
        ),
        in_specs=[smem, smem, smem, hbm],
        out_specs=(hbm, hbm, hbm),
        scratch_shapes=[
            pltpu.VMEM(desc_panel.shape, dt),
            pltpu.VMEM((PLANE, META, BR), dt),
            pltpu.SMEM((NA,), jnp.int32),
            pltpu.SMEM((NA,), jnp.int32),
            pltpu.SMEM((NA * SLOTS * 4 + count,), jnp.int32),
            pltpu.SemaphoreType.DMA((4,)),
            pltpu.SemaphoreType.DMA,
            pltpu.SemaphoreType.DMA,
            pltpu.SemaphoreType.DMA,
        ],
        name="pack",
    )(row_map.T, anc_order, anc_below.T, desc_panel)


GROUP = 8


def diag_kernel(codes, head_ref, out_ref):
    step = pl.program_id(0)

    @pl.when(step == 0)
    def _():
        out_ref[...] = jnp.zeros_like(out_ref)

    for g in range(GROUP):
        blocks = [head_ref[g, t * BR:(t + 1) * BR, :] for t in range(2 * SLOTS)]
        products = [nt_dot(block, block) for block in blocks]
        for t, product in enumerate(products):
            c = codes[step * GROUP + g, t * 3]
            place = jnp.where(c < CB, (t // SLOTS) * CB + c, 2 * CB)
            out_ref[place] = out_ref[place] + product


def diag_sums(codes, head):
    return pl.pallas_call(
        diag_kernel,
        out_shape=jax.ShapeDtypeStruct((2 * CB + 1, BR, BR), jnp.float32),
        grid_spec=pltpu.PrefetchScalarGridSpec(
            num_scalar_prefetch=1,
            grid=(PLANE // GROUP,),
            in_specs=[pl.BlockSpec((GROUP, HEAD_ROWS, BR), lambda k, codes: (k, 0, 0))],
            out_specs=pl.BlockSpec((2 * CB + 1, BR, BR), lambda k, codes: (0, 0, 0)),
        ),
        name="diag_sums",
    )(codes, head)


def below_kernel(i, codes, head_ref, tail_ref, out_ref):
    step = pl.program_id(0)

    @pl.when(step == 0)
    def _():
        out_ref[...] = jnp.zeros_like(out_ref)

    for g in range(GROUP):
        products = [
            nt_dot(tail_ref[g, s], head_ref[g, s * BR:(s + 1) * BR, :]) for s in range(SLOTS)
        ]
        for s, product in enumerate(products):
            t = i * SLOTS + s
            c = codes[step * GROUP + g, t * 3]
            for r in range(2):
                j = codes[step * GROUP + g, t * 3 + 1 + r]
                place = ((j % Y) * (Q // Y) + j // Y) * CB + c
                place = jnp.where(c < CB, place, BELOW)
                out_ref[place] = out_ref[place] + product[r * BR:(r + 1) * BR]


def below_sums(i, codes, head, tail):
    return pl.pallas_call(
        functools.partial(below_kernel, i),
        out_shape=jax.ShapeDtypeStruct((BELOW + PIECE, BR, BR), jnp.float32),
        grid_spec=pltpu.PrefetchScalarGridSpec(
            num_scalar_prefetch=1,
            grid=(PLANE // GROUP,),
            in_specs=[
                pl.BlockSpec((GROUP, SLOTS * BR, BR), lambda k, codes: (k, i, 0)),
                pl.BlockSpec((GROUP, SLOTS, 2 * BR, BR), lambda k, codes: (k, 0, 0, 0)),
            ],
            out_specs=pl.BlockSpec((BELOW + PIECE, BR, BR), lambda k, codes: (0, 0, 0)),
        ),
    )(codes, head, tail)


def nn_dot(a, b):
    return lax.dot_general(
        a, b, (((1,), (0,)), ((), ())), precision=HIGHEST, preferred_element_type=jnp.float32
    )


def tn_dot(a, b):
    return lax.dot_general(
        a, b, (((0,), (0,)), ((), ())), precision=HIGHEST, preferred_element_type=jnp.float32
    )


def factor_block(pair, between):
    sub = lax.broadcasted_iota(jnp.int32, (NB, BR), 0)
    sub2 = lax.broadcasted_iota(jnp.int32, (NB, 2 * BR), 0)
    lane = lax.broadcasted_iota(jnp.int32, (NB, BR), 1)
    for k in range(BR // NB):
        between(k)
        rows = pair[k * NB:(k + 1) * NB, :]
        cols = [jnp.broadcast_to(rows[:, k * NB + j:k * NB + j + 1], (NB, BR)) for j in range(NB)]
        for j in range(NB):
            scale = lax.rsqrt(cols[j][j:j + 1, :])
            column = cols[j] * scale
            below = jnp.where(sub > j, column, 0.0)
            row = rows[j:j + 1, :] * jnp.concatenate([scale, scale], axis=1)
            rows = jnp.where(sub2 == j, row, rows - jnp.concatenate([below, below], axis=1) * row)
            for m in range(j + 1, NB):
                cols[m] = cols[m] - below * column[m:m + 1, :]
        pair[k * NB:(k + 1) * NB, :] = rows
        start = (k + 1) * NB
        if start < BR:
            left = jnp.where(lane >= start, rows[:, :BR], 0.0)
            pair[start:, :] = pair[start:, :] - tn_dot(left, rows)[start:]


def factor_whole(lower_ref, inverse_ref, work, pair, between):
    width = work.shape[0]
    inverse_ref[...] = jnp.zeros_like(inverse_ref)
    row = lax.broadcasted_iota(jnp.int32, (BR, BR), 0)
    col = lax.broadcasted_iota(jnp.int32, (BR, BR), 1)
    all_rows = lax.broadcasted_iota(jnp.int32, (width, BR), 0)
    wide = lax.broadcasted_iota(jnp.int32, (BR, width), 1)
    high = lax.broadcasted_iota(jnp.int32, (BR, width), 0)

    def step(kb, carry):
        at = pl.ds(pl.multiple_of(kb * BR, BR), BR)
        pair[:, :BR] = work[at, at]
        pair[:, BR:] = jnp.where(row == col, 1.0, 0.0)
        factor_block(pair, functools.partial(between, kb))
        diagonal = jnp.where(col >= row, pair[:, :BR], 0.0).T
        small = jnp.where(col <= row, pair[:, BR:], 0.0)
        between(kb, BR // NB)
        panel = nt_dot(work[:, at], small, HIGHEST)
        panel = jnp.where(all_rows >= (kb + 1) * BR, panel, 0.0)
        lower_ref[:, at] = panel
        lower_ref[at, at] = diagonal
        work[...] = work[...] - nt_dot(panel, panel, HIGHEST)
        before = jnp.where(wide < kb * BR, lower_ref[at, :], 0.0)
        target = jnp.where(wide == high + kb * BR, 1.0, 0.0) - nn_dot(before, inverse_ref[...])
        inverse_ref[at, :] = nn_dot(small, target)
        return carry

    lax.fori_loop(0, width // BR, step, 0)


def remote(src, dst, send_sem, recv_sem, **device):
    return pltpu.make_async_remote_copy(
        src_ref=src, dst_ref=dst, send_sem=send_sem, recv_sem=recv_sem,
        device_id=device, device_id_type=pl.DeviceIdType.MESH,
    )


def signal(semaphore, **device):
    pl.semaphore_signal(
        semaphore, inc=1, device_id=device, device_id_type=pl.DeviceIdType.MESH
    )


def target_z(i, core, y):
    return y + Y * jnp.bitwise_xor(core, i)


def diag_reduce_kernel(sums, out, arrived, send_sems, recv_sems):
    z, y = lax.axis_index("z"), lax.axis_index("y")
    core = lax.axis_index("xc") % 2
    here = z % Y == y

    barrier = pltpu.get_barrier_semaphore()
    for source in range(Z):
        @pl.when(jnp.logical_and(here, source != z))
        def _():
            signal(barrier, z=jnp.int32(source))
    pl.semaphore_wait(barrier, 2 - here.astype(jnp.int32))

    def send(i):
        return remote(
            sums.at[pl.ds(i * CB, CB)], arrived.at[z], send_sems.at[i], recv_sems.at[z],
            z=target_z(i, core, y),
        )

    for i in range(2):
        @pl.when(target_z(i, core, y) != z)
        def _():
            send(i).start()

        @pl.when(target_z(i, core, y) == z)
        def _():
            arrived[z] = sums[i * CB:(i + 1) * CB]

    @pl.when(here)
    def _():
        for source in range(Z):
            @pl.when(source != z)
            def _():
                remote(
                    sums.at[pl.ds(0, CB)], arrived.at[source], send_sems.at[0],
                    recv_sems.at[source], z=(z + 1) % Z,
                ).wait_recv()
        update = arrived[0]
        for source in range(1, Z):
            update = update + arrived[source]
        out[...] = update

    @pl.when(jnp.logical_not(here))
    def _():
        out[...] = jnp.zeros_like(out)

    for i in range(2):
        @pl.when(target_z(i, core, y) != z)
        def _():
            send(i).wait_send()


def diag_reduce(sums):
    return pl.pallas_call(
        diag_reduce_kernel,
        out_shape=jax.ShapeDtypeStruct((CB, BR, BR), jnp.float32),
        in_specs=[IN_VMEM],
        out_specs=IN_VMEM,
        scratch_shapes=[
            pltpu.VMEM((Z, CB, BR, BR), jnp.float32),
            pltpu.SemaphoreType.DMA((2,)),
            pltpu.SemaphoreType.DMA((Z,)),
        ],
        compiler_params=pltpu.CompilerParams(collective_id=0, has_side_effects=True),
        name="diag_reduce",
    )(sums)


def spread_route(k):
    pairs = []
    for z in range(Z):
        for xc in range(XC):
            base = (z * XC + xc) * Y
            pairs.append((base + z % Y, base + (z + k) % Y))
    return pairs


class Chain:
    def __init__(self, i, sums, up, down, up_sems, down_sems, send_sem):
        self.z, self.y = lax.axis_index("z"), lax.axis_index("y")
        self.distance = (target_z(i, lax.axis_index("xc") % 2, self.y) - self.z + Z) % Z
        self.above, self.under = (self.z + 1) % Z, (self.z + Z - 1) % Z
        self.sums, self.up, self.down = sums, up, down
        self.up_sems, self.down_sems, self.send_sem = up_sems, down_sems, send_sem

    def meet(self, barrier):
        signal(barrier, z=self.above)
        signal(barrier, z=self.under)

    def copy(self, source, buffer, sems, q, to):
        return remote(source.at[q], buffer.at[q], self.send_sem, sems.at[q], z=to)

    def begin(self):
        for distance, buffer, sems, to in (
            (4, self.up, self.up_sems, self.above), (5, self.down, self.down_sems, self.under)
        ):
            @pl.when(self.distance == distance)
            def _():
                def body(q, carry):
                    self.copy(self.sums, buffer, sems, q, to).start()
                    return carry

                lax.fori_loop(0, PIECES, body, 0)

    def advance(self, q, deliver):
        for some, buffer, sems, to in (
            (jnp.logical_and(self.distance >= 1, self.distance <= 3),
             self.up, self.up_sems, self.above),
            (self.distance >= 6, self.down, self.down_sems, self.under),
        ):
            @pl.when(some)
            def _():
                self.copy(self.sums, buffer, sems, q, to).wait_recv()
                buffer[q] = buffer[q] + self.sums[q]
                self.copy(buffer, buffer, sems, q, to).start()

        @pl.when(self.distance == 0)
        def _():
            self.copy(self.sums, self.up, self.up_sems, q, self.above).wait_recv()
            self.copy(self.sums, self.down, self.down_sems, q, self.above).wait_recv()
            deliver(q, self.up[q] + self.down[q] + self.sums[q])

    def finish(self):
        @pl.when(self.distance != 0)
        def _():
            remote(self.up, self.up, self.send_sem, self.up_sems.at[0], z=self.above).wait_send()


CHAIN_SCRATCH = [
    pltpu.VMEM((PIECES, PIECE, BR, BR), jnp.float32),
    pltpu.VMEM((PIECES, PIECE, BR, BR), jnp.float32),
    pltpu.SemaphoreType.DMA((PIECES,)),
    pltpu.SemaphoreType.DMA((PIECES,)),
    pltpu.SemaphoreType.DMA,
]
IN_VMEM = pl.BlockSpec(memory_space=pltpu.VMEM)


def first_kernel(
    sums, strip, strip1, strip2, strip3, part, part1, part2, part3, total, lower, inverse,
    up, down, up_sems, down_sems, send_sem, work, pair, strips,
):
    chain = Chain(0, sums, up, down, up_sems, down_sems, send_sem)
    y = chain.y
    barrier = pltpu.get_barrier_semaphore()
    chain.meet(barrier)
    pl.semaphore_wait(barrier, 2)
    chain.begin()

    for k, one in enumerate((strip, strip1, strip2, strip3)):
        strips[(y + Y - k) % Y] = one[...]
    work[...] = jnp.zeros_like(work)
    blocks = {(1, 0): strips[1, 0], (2, 1): strips[2, 0], (3, 2): strips[3, 0],
              (3, 0): strips[0, 0].T, (2, 0): strips[2, 1], (3, 1): strips[3, 1]}
    for c in range(CB):
        blocks[c, c] = strips[c, 2] - (part[c] + part1[c] + part2[c] + part3[c])
    for (b, c), block in blocks.items():
        work[b * BR:(b + 1) * BR, c * BR:(c + 1) * BR] = block

    def deliver(q, value):
        total[q] = value

    turns = (0, 2, 3, 5, 6, BR // NB)

    def between(kb, k):
        if k in turns:
            chain.advance(kb * len(turns) + turns.index(k), deliver)

    factor_whole(lower, inverse, work, pair, between)
    chain.finish()


def first_reduce(sums, strips, parts):
    width = CB * BR
    shape = jax.ShapeDtypeStruct((width, width), jnp.float32)
    return pl.pallas_call(
        first_kernel,
        out_shape=(jax.ShapeDtypeStruct((PIECES, PIECE, BR, BR), jnp.float32), shape, shape),
        in_specs=[IN_VMEM] * (1 + 2 * Y),
        out_specs=(IN_VMEM,) * 3,
        scratch_shapes=CHAIN_SCRATCH + [
            pltpu.VMEM((width, width), jnp.float32),
            pltpu.VMEM((BR, 2 * BR), jnp.float32),
            pltpu.VMEM((Y, 3, BR, BR), jnp.float32),
        ],
        compiler_params=pltpu.CompilerParams(collective_id=1, has_side_effects=True),
        name="first_reduce",
    )(sums.reshape(PIECES + 1, PIECE, BR, BR), *strips, *parts)


def second_kernel(
    sums, total, out, up, down, up_sems, down_sems, send_sem, final, final_sems, spread_sem
):
    chain = Chain(1, sums, up, down, up_sems, down_sems, send_sem)
    z, y = chain.z, chain.y
    has_first = chain.distance == 4
    own = PIECES // Y
    barrier = pltpu.get_barrier_semaphore()
    chain.meet(barrier)
    for k in range(1, Y):
        signal(barrier, y=(y + k) % Y)
    pl.semaphore_wait(barrier, Y + 1)
    chain.begin()

    def spread(source, q):
        return remote(source.at[q], final.at[q % own], spread_sem, final_sems.at[q % own], y=q // own)

    @pl.when(has_first)
    def _():
        def body(q, carry):
            @pl.when(q // own == y)
            def _():
                out[q % own] = total[q]

            @pl.when(q // own != y)
            def _():
                spread(total, q).start()

            return carry

        lax.fori_loop(0, PIECES, body, 0)

    def deliver(q, value):
        @pl.when(q // own == y)
        def _():
            out[q % own] = value

        @pl.when(q // own != y)
        def _():
            up[q] = value
            spread(up, q).start()

    def body(q, carry):
        chain.advance(q, deliver)
        return carry

    lax.fori_loop(0, PIECES, body, 0)
    chain.finish()

    @pl.when(z % Y == y)
    def _():
        part = up.at[pl.ds(0, PIECES - own)]
        remote(part, part, spread_sem, up_sems.at[0], z=chain.above).wait_send()

    @pl.when(z % Y != y)
    def _():
        def body(place, carry):
            chain.copy(sums, final, final_sems, place, chain.above).wait_recv()
            out[place] = final[place]
            return carry

        lax.fori_loop(0, own, body, 0)


def second_reduce(sums, total):
    own = PIECES // Y
    return pl.pallas_call(
        second_kernel,
        out_shape=jax.ShapeDtypeStruct((own, PIECE, BR, BR), jnp.float32),
        in_specs=[IN_VMEM] * 2,
        out_specs=IN_VMEM,
        scratch_shapes=CHAIN_SCRATCH + [
            pltpu.VMEM((own, PIECE, BR, BR), jnp.float32),
            pltpu.SemaphoreType.DMA((own,)),
            pltpu.SemaphoreType.DMA,
        ],
        compiler_params=pltpu.CompilerParams(collective_id=2, has_side_effects=True),
        name="second_reduce",
    )(sums.reshape(PIECES + 1, PIECE, BR, BR), total)


def solve_kernel(y_ref, rows_ref, lower_ref, inverse_ref, update_ref, out_ref):
    m = pl.program_id(0)

    @pl.when(m == 0)
    def _():
        out_ref[0, 0, 0] = lower_ref[...]

    @pl.when(m > 0)
    def _():
        update = jnp.concatenate([update_ref[0, c] for c in range(CB)], axis=1)
        out_ref[0, 0, 0] = nt_dot(rows_ref[0, 0, 0] - update, inverse_ref[...], HIGHEST)


def solve(anc_panel, lower, inverse, update, y):
    width = anc_panel.shape[4]
    update = update.reshape(Q // Y, CB, BR, BR)
    return pl.pallas_call(
        solve_kernel,
        out_shape=jax.ShapeDtypeStruct(anc_panel.shape, jnp.float32),
        grid_spec=pltpu.PrefetchScalarGridSpec(
            num_scalar_prefetch=1,
            grid=(anc_panel.shape[1],),
            in_specs=[
                pl.BlockSpec((1, 1, 1, BR, width), lambda m, y: (0, m, 0, 0, 0)),
                pl.BlockSpec((BR, width), lambda m, y: (y[0], 0)),
                pl.BlockSpec((width, width), lambda m, y: (0, 0)),
                pl.BlockSpec((1, CB, BR, BR), lambda m, y: (jnp.maximum(m - 1, 0), 0, 0, 0)),
            ],
            out_specs=pl.BlockSpec((1, 1, 1, BR, width), lambda m, y: (0, m, 0, 0, 0)),
        ),
        name="solve",
    )(y, anc_panel, lower, inverse, update)


def exchange(value):
    return lax.all_to_all(value, ("xc", "y"), split_axis=0, concat_axis=0, tiled=True)


def strip_blocks(anc_panel, y):
    strip = anc_panel[0, 0, 0]
    columns = [lax.rem(y + Y - 1, Y), lax.rem(y + 2, Y), y]
    zero = jnp.int32(0)
    return jnp.stack(
        [lax.dynamic_slice(strip, (zero, c * BR), (BR, BR), allow_negative_indices=False) for c in columns]
    )


def shards(desc_panel, row_map, anc_order, anc_below, anc_panel):
    y = lax.axis_index("y").astype(jnp.int32)
    head, tail0, tail1 = pack(row_map, anc_order, anc_below, desc_panel)
    head = exchange(head)
    tail0, head, anc_panel = lax.optimization_barrier((tail0, head, anc_panel))
    tail0 = exchange(tail0)
    codes = head[:, 2 * SLOTS * BR, : 2 * SLOTS * 3].astype(jnp.int32)
    part = diag_reduce(diag_sums(codes, head))
    strip = strip_blocks(anc_panel, y)
    strips, parts = [strip], [part]
    for k in range(1, Y):
        strips.append(lax.ppermute(strip, "y", [(b, (b + k) % Y) for b in range(Y)]))
    for k in range(1, Y):
        parts.append(lax.ppermute(part, ALL, spread_route(k)))
    tail1, tail0, part = lax.optimization_barrier((tail1, tail0, part))
    tail1 = exchange(tail1)
    total, lower, inverse = first_reduce(below_sums(0, codes, head, tail0), strips, parts)
    tail1, total = lax.optimization_barrier((tail1, total))
    update = second_reduce(below_sums(1, codes, head, tail1), total)
    return solve(anc_panel, lower, inverse, update, y.reshape(1))


def solution(mesh):
    grid = Mesh(mesh.devices.reshape(Z, XC, Y), ALL)
    in_specs = (
        P(ALL, None, None),
        P(ALL, None),
        P(),
        P(),
        P(("z", "xc"), None, "y", None, None),
    )
    out_specs = P(("z", "xc"), None, "y", None, None)
    return jax.shard_map(
        shards, mesh=grid, in_specs=in_specs, out_specs=out_specs, check_vma=False
    )
```

```python
import functools

import jax
import jax.numpy as jnp
from jax import lax
from jax.experimental import pallas as pl
from jax.experimental.pallas import tpu as pltpu
from jax.sharding import Mesh
from jax.sharding import PartitionSpec as P

Z, XC, Y = 8, 8, 4
PLANE = XC * Y
BR = 128
CB = 4
Q = 12
SLOTS = 2
NA = 64
NONE = 7
META = 16
HEAD_ROWS = 2 * SLOTS * BR + META
BELOW = Q * CB
HIGHEST = lax.Precision.HIGHEST
NB = 16
PIECE = 2
PIECES = BELOW // PIECE
ALL = ("z", "xc", "y")


def nt_dot(a, b, precision=None):
    return lax.dot_general(
        a, b, (((1,), (1,)), ((), ())), precision=precision, preferred_element_type=jnp.float32
    )


def pack_kernel(
    map_ref, order_ref, below_ref, desc_ref, head_ref, tail0_ref, tail1_ref,
    stage, meta, inverse, used, codes, in_sems, head_sem, tail_sem, meta_sem,
):
    count = map_ref.shape[1]
    parts = in_sems.shape[0]
    step = count // parts

    def load(k):
        part = pl.ds(k * step, step)
        return pltpu.make_async_copy(desc_ref.at[part], stage.at[part], in_sems.at[k])

    for k in range(parts):
        load(k).start()

    def clear(a, carry):
        inverse[order_ref[a]] = a
        used[a] = 0
        for s in range(SLOTS):
            codes[(a * SLOTS + s) * 4] = NONE
            codes[(a * SLOTS + s) * 4 + 1] = 0
            codes[(a * SLOTS + s) * 4 + 2] = 0
        return carry

    lax.fori_loop(0, NA, clear, 0)

    def route(d, carry):
        head = map_ref[0, d]
        a = inverse[head // CB]
        s = used[a]
        used[a] = s + 1
        dest = (a % XC) * Y + (a // XC) % Y
        i = jnp.bitwise_xor(a // (XC * Y), a % 2)
        slot = (dest * 2 + i) * SLOTS + s
        first, second = map_ref[1, d], map_ref[2, d]
        j1, j2 = jnp.int32(0), jnp.int32(0)
        for j in range(Q):
            g = below_ref[j, a]
            j1 = jnp.where(g == first, j, j1)
            j2 = jnp.where(g == second, j, j2)
        codes[slot * 4] = head % CB
        codes[slot * 4 + 1] = j1
        codes[slot * 4 + 2] = j2
        codes[NA * SLOTS * 4 + d] = slot
        return carry

    lax.fori_loop(0, count, route, 0)

    lane = lax.broadcasted_iota(jnp.int32, (META, 128), 1)

    def describe(dest, carry):
        row = jnp.zeros((META, 128), jnp.int32)
        for t in range(2 * SLOTS):
            for f in range(3):
                row = jnp.where(lane == t * 3 + f, codes[(dest * 2 * SLOTS + t) * 4 + f], row)
        meta[dest] = row.astype(jnp.float32).astype(jnp.bfloat16)
        return carry

    lax.fori_loop(0, PLANE, describe, 0)

    for k in range(parts):
        load(k).wait()

    def send_head(d, carry):
        slot = codes[NA * SLOTS * 4 + d]
        place = pl.multiple_of((slot % (2 * SLOTS)) * BR, BR)
        pltpu.make_async_copy(
            stage.at[d, pl.ds(0, BR)],
            head_ref.at[slot // (2 * SLOTS), pl.ds(place, BR)],
            head_sem,
        ).start()
        return carry

    lax.fori_loop(0, count, send_head, 0)
    pltpu.make_async_copy(meta, head_ref.at[:, pl.ds(2 * SLOTS * BR, META)], meta_sem).start()

    def send_tail(d, carry):
        slot = codes[NA * SLOTS * 4 + d]
        dest, i, s = slot // (2 * SLOTS), (slot // SLOTS) % 2, slot % SLOTS
        for k, out in ((0, tail0_ref), (1, tail1_ref)):
            @pl.when(i == k)
            def _():
                pltpu.make_async_copy(
                    stage.at[d, pl.ds(BR, 2 * BR)], out.at[dest, s], tail_sem
                ).start()
        return carry

    lax.fori_loop(0, count, send_tail, 0)
    pltpu.make_async_copy(meta, head_ref.at[:, pl.ds(2 * SLOTS * BR, META)], meta_sem).wait()
    heads = stage.at[:, pl.ds(0, BR)]
    pltpu.make_async_copy(heads, heads, head_sem).wait()
    tails = stage.at[:, pl.ds(BR, 2 * BR)]
    pltpu.make_async_copy(tails, tails, tail_sem).wait()


def pack(row_map, anc_order, anc_below, desc_panel):
    count = row_map.shape[0]
    smem = pl.BlockSpec(memory_space=pltpu.SMEM)
    hbm = pl.BlockSpec(memory_space=pltpu.HBM)
    dt = desc_panel.dtype
    return pl.pallas_call(
        pack_kernel,
        out_shape=(
            jax.ShapeDtypeStruct((PLANE, HEAD_ROWS, BR), dt),
            jax.ShapeDtypeStruct((PLANE, SLOTS, 2 * BR, BR), dt),
            jax.ShapeDtypeStruct((PLANE, SLOTS, 2 * BR, BR), dt),
        ),
        in_specs=[smem, smem, smem, hbm],
        out_specs=(hbm, hbm, hbm),
        scratch_shapes=[
            pltpu.VMEM(desc_panel.shape, dt),
            pltpu.VMEM((PLANE, META, BR), dt),
            pltpu.SMEM((NA,), jnp.int32),
            pltpu.SMEM((NA,), jnp.int32),
            pltpu.SMEM((NA * SLOTS * 4 + count,), jnp.int32),
            pltpu.SemaphoreType.DMA((4,)),
            pltpu.SemaphoreType.DMA,
            pltpu.SemaphoreType.DMA,
            pltpu.SemaphoreType.DMA,
        ],
        name="pack",
    )(row_map.T, anc_order, anc_below.T, desc_panel)


GROUP = 8


def diag_kernel(codes, head_ref, out_ref):
    step = pl.program_id(0)

    @pl.when(step == 0)
    def _():
        out_ref[...] = jnp.zeros_like(out_ref)

    for g in range(GROUP):
        blocks = [head_ref[g, t * BR:(t + 1) * BR, :] for t in range(2 * SLOTS)]
        products = [nt_dot(block, block) for block in blocks]
        for t, product in enumerate(products):
            c = codes[step * GROUP + g, t * 3]
            place = jnp.where(c < CB, (t // SLOTS) * CB + c, 2 * CB)
            out_ref[place] = out_ref[place] + product


def diag_sums(codes, head):
    return pl.pallas_call(
        diag_kernel,
        out_shape=jax.ShapeDtypeStruct((2 * CB + 1, BR, BR), jnp.float32),
        grid_spec=pltpu.PrefetchScalarGridSpec(
            num_scalar_prefetch=1,
            grid=(PLANE // GROUP,),
            in_specs=[pl.BlockSpec((GROUP, HEAD_ROWS, BR), lambda k, codes: (k, 0, 0))],
            out_specs=pl.BlockSpec((2 * CB + 1, BR, BR), lambda k, codes: (0, 0, 0)),
        ),
        name="diag_sums",
    )(codes, head)


def below_kernel(i, codes, head_ref, tail_ref, out_ref):
    step = pl.program_id(0)

    @pl.when(step == 0)
    def _():
        out_ref[...] = jnp.zeros_like(out_ref)

    for g in range(GROUP):
        products = [
            nt_dot(tail_ref[g, s], head_ref[g, s * BR:(s + 1) * BR, :]) for s in range(SLOTS)
        ]
        for s, product in enumerate(products):
            t = i * SLOTS + s
            c = codes[step * GROUP + g, t * 3]
            for r in range(2):
                j = codes[step * GROUP + g, t * 3 + 1 + r]
                place = ((j % Y) * (Q // Y) + j // Y) * CB + c
                place = jnp.where(c < CB, place, BELOW)
                out_ref[place] = out_ref[place] + product[r * BR:(r + 1) * BR]


def below_sums(i, codes, head, tail):
    return pl.pallas_call(
        functools.partial(below_kernel, i),
        out_shape=jax.ShapeDtypeStruct((BELOW + PIECE, BR, BR), jnp.float32),
        grid_spec=pltpu.PrefetchScalarGridSpec(
            num_scalar_prefetch=1,
            grid=(PLANE // GROUP,),
            in_specs=[
                pl.BlockSpec((GROUP, SLOTS * BR, BR), lambda k, codes: (k, i, 0)),
                pl.BlockSpec((GROUP, SLOTS, 2 * BR, BR), lambda k, codes: (k, 0, 0, 0)),
            ],
            out_specs=pl.BlockSpec((BELOW + PIECE, BR, BR), lambda k, codes: (0, 0, 0)),
        ),
    )(codes, head, tail)


def nn_dot(a, b):
    return lax.dot_general(
        a, b, (((1,), (0,)), ((), ())), precision=HIGHEST, preferred_element_type=jnp.float32
    )


def tn_dot(a, b):
    return lax.dot_general(
        a, b, (((0,), (0,)), ((), ())), precision=HIGHEST, preferred_element_type=jnp.float32
    )


def factor_block(pair, between):
    sub = lax.broadcasted_iota(jnp.int32, (NB, BR), 0)
    sub2 = lax.broadcasted_iota(jnp.int32, (NB, 2 * BR), 0)
    lane = lax.broadcasted_iota(jnp.int32, (NB, BR), 1)
    for k in range(BR // NB):
        between(k)
        rows = pair[k * NB:(k + 1) * NB, :]
        cols = [jnp.broadcast_to(rows[:, k * NB + j:k * NB + j + 1], (NB, BR)) for j in range(NB)]
        for j in range(NB):
            scale = lax.rsqrt(cols[j][j:j + 1, :])
            column = cols[j] * scale
            below = jnp.where(sub > j, column, 0.0)
            row = rows[j:j + 1, :] * jnp.concatenate([scale, scale], axis=1)
            rows = jnp.where(sub2 == j, row, rows - jnp.concatenate([below, below], axis=1) * row)
            for m in range(j + 1, NB):
                cols[m] = cols[m] - below * column[m:m + 1, :]
        pair[k * NB:(k + 1) * NB, :] = rows
        start = (k + 1) * NB
        if start < BR:
            left = jnp.where(lane >= start, rows[:, :BR], 0.0)
            pair[start:, :] = pair[start:, :] - tn_dot(left, rows)[start:]


def factor_whole(lower_ref, inverse_ref, work, pair, between):
    width = work.shape[0]
    inverse_ref[...] = jnp.zeros_like(inverse_ref)
    row = lax.broadcasted_iota(jnp.int32, (BR, BR), 0)
    col = lax.broadcasted_iota(jnp.int32, (BR, BR), 1)
    all_rows = lax.broadcasted_iota(jnp.int32, (width, BR), 0)
    wide = lax.broadcasted_iota(jnp.int32, (BR, width), 1)
    high = lax.broadcasted_iota(jnp.int32, (BR, width), 0)

    def step(kb, carry):
        at = pl.ds(pl.multiple_of(kb * BR, BR), BR)
        pair[:, :BR] = work[at, at]
        pair[:, BR:] = jnp.where(row == col, 1.0, 0.0)
        factor_block(pair, functools.partial(between, kb))
        diagonal = jnp.where(col >= row, pair[:, :BR], 0.0).T
        small = jnp.where(col <= row, pair[:, BR:], 0.0)
        between(kb, BR // NB)
        panel = nt_dot(work[:, at], small, HIGHEST)
        panel = jnp.where(all_rows >= (kb + 1) * BR, panel, 0.0)
        lower_ref[:, at] = panel
        lower_ref[at, at] = diagonal
        work[...] = work[...] - nt_dot(panel, panel, HIGHEST)
        between(kb, BR // NB + 1)
        before = jnp.where(wide < kb * BR, lower_ref[at, :], 0.0)
        target = jnp.where(wide == high + kb * BR, 1.0, 0.0) - nn_dot(before, inverse_ref[...])
        inverse_ref[at, :] = nn_dot(small, target)
        return carry

    lax.fori_loop(0, width // BR, step, 0)


def remote(src, dst, send_sem, recv_sem, **device):
    return pltpu.make_async_remote_copy(
        src_ref=src, dst_ref=dst, send_sem=send_sem, recv_sem=recv_sem,
        device_id=device, device_id_type=pl.DeviceIdType.MESH,
    )


def signal(semaphore, **device):
    pl.semaphore_signal(
        semaphore, inc=1, device_id=device, device_id_type=pl.DeviceIdType.MESH
    )


def target_z(i, core, y):
    return y + Y * jnp.bitwise_xor(core, i)


def diag_reduce_kernel(sums, out, arrived, send_sems, recv_sems):
    z, y = lax.axis_index("z"), lax.axis_index("y")
    core = lax.axis_index("xc") % 2
    here = z % Y == y

    barrier = pltpu.get_barrier_semaphore()
    for source in range(Z):
        @pl.when(jnp.logical_and(here, source != z))
        def _():
            signal(barrier, z=jnp.int32(source))
    pl.semaphore_wait(barrier, 2 - here.astype(jnp.int32))

    def send(i):
        return remote(
            sums.at[pl.ds(i * CB, CB)], arrived.at[z], send_sems.at[i], recv_sems.at[z],
            z=target_z(i, core, y),
        )

    for i in range(2):
        @pl.when(target_z(i, core, y) != z)
        def _():
            send(i).start()

        @pl.when(target_z(i, core, y) == z)
        def _():
            arrived[z] = sums[i * CB:(i + 1) * CB]

    @pl.when(here)
    def _():
        for source in range(Z):
            @pl.when(source != z)
            def _():
                remote(
                    sums.at[pl.ds(0, CB)], arrived.at[source], send_sems.at[0],
                    recv_sems.at[source], z=(z + 1) % Z,
                ).wait_recv()
        update = arrived[0]
        for source in range(1, Z):
            update = update + arrived[source]
        out[...] = update

    @pl.when(jnp.logical_not(here))
    def _():
        out[...] = jnp.zeros_like(out)

    for i in range(2):
        @pl.when(target_z(i, core, y) != z)
        def _():
            send(i).wait_send()


def diag_reduce(sums):
    return pl.pallas_call(
        diag_reduce_kernel,
        out_shape=jax.ShapeDtypeStruct((CB, BR, BR), jnp.float32),
        in_specs=[IN_VMEM],
        out_specs=IN_VMEM,
        scratch_shapes=[
            pltpu.VMEM((Z, CB, BR, BR), jnp.float32),
            pltpu.SemaphoreType.DMA((2,)),
            pltpu.SemaphoreType.DMA((Z,)),
        ],
        compiler_params=pltpu.CompilerParams(collective_id=0, has_side_effects=True),
        name="diag_reduce",
    )(sums)


def spread_route(k):
    pairs = []
    for z in range(Z):
        for xc in range(XC):
            base = (z * XC + xc) * Y
            pairs.append((base + z % Y, base + (z + k) % Y))
    return pairs


class Chain:
    def __init__(self, i, sums, up, down, up_sems, down_sems, send_sem):
        self.z, self.y = lax.axis_index("z"), lax.axis_index("y")
        self.distance = (target_z(i, lax.axis_index("xc") % 2, self.y) - self.z + Z) % Z
        self.above, self.under = (self.z + 1) % Z, (self.z + Z - 1) % Z
        self.sums, self.up, self.down = sums, up, down
        self.up_sems, self.down_sems, self.send_sem = up_sems, down_sems, send_sem

    def meet(self, barrier):
        signal(barrier, z=self.above)
        signal(barrier, z=self.under)

    def copy(self, source, buffer, sems, q, to):
        return remote(source.at[q], buffer.at[q], self.send_sem, sems.at[q], z=to)

    def begin(self):
        for distance, buffer, sems, to in (
            (4, self.up, self.up_sems, self.above), (5, self.down, self.down_sems, self.under)
        ):
            @pl.when(self.distance == distance)
            def _():
                def body(q, carry):
                    self.copy(self.sums, buffer, sems, q, to).start()
                    return carry

                lax.fori_loop(0, PIECES, body, 0)

    def advance(self, q, deliver):
        for some, buffer, sems, to in (
            (jnp.logical_and(self.distance >= 1, self.distance <= 3),
             self.up, self.up_sems, self.above),
            (self.distance >= 6, self.down, self.down_sems, self.under),
        ):
            @pl.when(some)
            def _():
                self.copy(self.sums, buffer, sems, q, to).wait_recv()
                buffer[q] = buffer[q] + self.sums[q]
                self.copy(buffer, buffer, sems, q, to).start()

        @pl.when(self.distance == 0)
        def _():
            self.copy(self.sums, self.up, self.up_sems, q, self.above).wait_recv()
            self.copy(self.sums, self.down, self.down_sems, q, self.above).wait_recv()
            deliver(q, self.up[q] + self.down[q] + self.sums[q])

    def finish(self):
        @pl.when(self.distance != 0)
        def _():
            remote(self.up, self.up, self.send_sem, self.up_sems.at[0], z=self.above).wait_send()


CHAIN_SCRATCH = [
    pltpu.VMEM((PIECES, PIECE, BR, BR), jnp.float32),
    pltpu.VMEM((PIECES, PIECE, BR, BR), jnp.float32),
    pltpu.SemaphoreType.DMA((PIECES,)),
    pltpu.SemaphoreType.DMA((PIECES,)),
    pltpu.SemaphoreType.DMA,
]
IN_VMEM = pl.BlockSpec(memory_space=pltpu.VMEM)


def first_kernel(sums, total, up, down, up_sems, down_sems, send_sem):
    chain = Chain(0, sums, up, down, up_sems, down_sems, send_sem)
    barrier = pltpu.get_barrier_semaphore()
    chain.meet(barrier)
    pl.semaphore_wait(barrier, 2)
    chain.begin()

    def deliver(q, value):
        total[q] = value

    def body(q, carry):
        chain.advance(q, deliver)
        return carry

    lax.fori_loop(0, PIECES, body, 0)
    chain.finish()


def first_reduce(sums):
    return pl.pallas_call(
        first_kernel,
        out_shape=jax.ShapeDtypeStruct((PIECES, PIECE, BR, BR), jnp.float32),
        in_specs=[IN_VMEM],
        out_specs=IN_VMEM,
        scratch_shapes=CHAIN_SCRATCH,
        compiler_params=pltpu.CompilerParams(collective_id=1, has_side_effects=True),
        name="first_reduce",
    )(sums.reshape(PIECES + 1, PIECE, BR, BR))


def second_kernel(
    sums, total, strip, strip1, strip2, strip3, part, part1, part2, part3, out, lower, inverse,
    up, down, up_sems, down_sems, send_sem, final, final_sems, spread_sem, work, pair, strips,
):
    chain = Chain(1, sums, up, down, up_sems, down_sems, send_sem)
    z, y = chain.z, chain.y
    has_first = chain.distance == 4
    own = PIECES // Y
    barrier = pltpu.get_barrier_semaphore()
    chain.meet(barrier)
    for k in range(1, Y):
        signal(barrier, y=(y + k) % Y)
    pl.semaphore_wait(barrier, Y + 1)
    chain.begin()

    def spread(source, q):
        return remote(source.at[q], final.at[q % own], spread_sem, final_sems.at[q % own], y=q // own)

    @pl.when(has_first)
    def _():
        def body(q, carry):
            @pl.when(q // own == y)
            def _():
                out[q % own] = total[q]

            @pl.when(q // own != y)
            def _():
                spread(total, q).start()

            return carry

        lax.fori_loop(0, PIECES, body, 0)

    def deliver(q, value):
        @pl.when(q // own == y)
        def _():
            out[q % own] = value

        @pl.when(q // own != y)
        def _():
            up[q] = value
            spread(up, q).start()

    for k, one in enumerate((strip, strip1, strip2, strip3)):
        strips[(y + Y - k) % Y] = one[...]
    work[...] = jnp.zeros_like(work)
    blocks = {(1, 0): strips[1, 0], (2, 1): strips[2, 0], (3, 2): strips[3, 0],
              (3, 0): strips[0, 0].T, (2, 0): strips[2, 1], (3, 1): strips[3, 1]}
    for c in range(CB):
        blocks[c, c] = strips[c, 2] - (part[c] + part1[c] + part2[c] + part3[c])
    for (b, c), block in blocks.items():
        work[b * BR:(b + 1) * BR, c * BR:(c + 1) * BR] = block

    turns = (0, 2, 4, 6, BR // NB, BR // NB + 1)

    def between(kb, k):
        if k in turns:
            chain.advance(kb * len(turns) + turns.index(k), deliver)

    factor_whole(lower, inverse, work, pair, between)
    chain.finish()

    @pl.when(z % Y == y)
    def _():
        part = up.at[pl.ds(0, PIECES - own)]
        remote(part, part, spread_sem, up_sems.at[0], z=chain.above).wait_send()

    @pl.when(z % Y != y)
    def _():
        def body(place, carry):
            chain.copy(sums, final, final_sems, place, chain.above).wait_recv()
            out[place] = final[place]
            return carry

        lax.fori_loop(0, own, body, 0)


def second_reduce(sums, total, strips, parts):
    own, width = PIECES // Y, CB * BR
    square = jax.ShapeDtypeStruct((width, width), jnp.float32)
    return pl.pallas_call(
        second_kernel,
        out_shape=(jax.ShapeDtypeStruct((own, PIECE, BR, BR), jnp.float32), square, square),
        in_specs=[IN_VMEM] * (2 + 2 * Y),
        out_specs=(IN_VMEM,) * 3,
        scratch_shapes=CHAIN_SCRATCH + [
            pltpu.VMEM((own, PIECE, BR, BR), jnp.float32),
            pltpu.SemaphoreType.DMA((own,)),
            pltpu.SemaphoreType.DMA,
            pltpu.VMEM((width, width), jnp.float32),
            pltpu.VMEM((BR, 2 * BR), jnp.float32),
            pltpu.VMEM((Y, 3, BR, BR), jnp.float32),
        ],
        compiler_params=pltpu.CompilerParams(collective_id=2, has_side_effects=True),
        name="second_reduce",
    )(sums.reshape(PIECES + 1, PIECE, BR, BR), total, *strips, *parts)


def solve_kernel(y_ref, rows_ref, lower_ref, inverse_ref, update_ref, out_ref):
    m = pl.program_id(0)

    @pl.when(m == 0)
    def _():
        out_ref[0, 0, 0] = lower_ref[...]

    @pl.when(m > 0)
    def _():
        update = jnp.concatenate([update_ref[0, c] for c in range(CB)], axis=1)
        out_ref[0, 0, 0] = nt_dot(rows_ref[0, 0, 0] - update, inverse_ref[...], HIGHEST)


def solve(anc_panel, lower, inverse, update, y):
    width = anc_panel.shape[4]
    update = update.reshape(Q // Y, CB, BR, BR)
    return pl.pallas_call(
        solve_kernel,
        out_shape=jax.ShapeDtypeStruct(anc_panel.shape, jnp.float32),
        grid_spec=pltpu.PrefetchScalarGridSpec(
            num_scalar_prefetch=1,
            grid=(anc_panel.shape[1],),
            in_specs=[
                pl.BlockSpec((1, 1, 1, BR, width), lambda m, y: (0, m, 0, 0, 0)),
                pl.BlockSpec((BR, width), lambda m, y: (y[0], 0)),
                pl.BlockSpec((width, width), lambda m, y: (0, 0)),
                pl.BlockSpec((1, CB, BR, BR), lambda m, y: (jnp.maximum(m - 1, 0), 0, 0, 0)),
            ],
            out_specs=pl.BlockSpec((1, 1, 1, BR, width), lambda m, y: (0, m, 0, 0, 0)),
        ),
        name="solve",
    )(y, anc_panel, lower, inverse, update)


def exchange(value):
    return lax.all_to_all(value, ("xc", "y"), split_axis=0, concat_axis=0, tiled=True)


def strip_blocks(anc_panel, y):
    strip = anc_panel[0, 0, 0]
    columns = [lax.rem(y + Y - 1, Y), lax.rem(y + 2, Y), y]
    zero = jnp.int32(0)
    return jnp.stack(
        [lax.dynamic_slice(strip, (zero, c * BR), (BR, BR), allow_negative_indices=False) for c in columns]
    )


def shards(desc_panel, row_map, anc_order, anc_below, anc_panel):
    y = lax.axis_index("y").astype(jnp.int32)
    head, tail0, tail1 = pack(row_map, anc_order, anc_below, desc_panel)
    head = exchange(head)
    tail0, head, anc_panel = lax.optimization_barrier((tail0, head, anc_panel))
    tail0 = exchange(tail0)
    codes = head[:, 2 * SLOTS * BR, : 2 * SLOTS * 3].astype(jnp.int32)
    part = diag_reduce(diag_sums(codes, head))
    strip = strip_blocks(anc_panel, y)
    strips, parts = [strip], [part]
    for k in range(1, Y):
        strips.append(lax.ppermute(strip, "y", [(b, (b + k) % Y) for b in range(Y)]))
    for k in range(1, Y):
        parts.append(lax.ppermute(part, ALL, spread_route(k)))
    tail1, tail0, part = lax.optimization_barrier((tail1, tail0, part))
    tail1 = exchange(tail1)
    total = first_reduce(below_sums(0, codes, head, tail0))
    tail1, total = lax.optimization_barrier((tail1, total))
    sums = below_sums(1, codes, head, tail1)
    update, lower, inverse = second_reduce(sums, total, strips, parts)
    return solve(anc_panel, lower, inverse, update, y.reshape(1))


def solution(mesh):
    grid = Mesh(mesh.devices.reshape(Z, XC, Y), ALL)
    in_specs = (
        P(ALL, None, None),
        P(ALL, None),
        P(),
        P(),
        P(("z", "xc"), None, "y", None, None),
    )
    out_specs = P(("z", "xc"), None, "y", None, None)
    return jax.shard_map(
        shards, mesh=grid, in_specs=in_specs, out_specs=out_specs, check_vma=False
    )
```

```python
import functools

import jax
import jax.numpy as jnp
from jax import lax
from jax.experimental import pallas as pl
from jax.experimental.pallas import tpu as pltpu
from jax.sharding import Mesh
from jax.sharding import PartitionSpec as P

Z, XC, Y = 8, 8, 4
PLANE = XC * Y
BR = 128
CB = 4
Q = 12
SLOTS = 2
NA = 64
NONE = 7
META = 16
HEAD_ROWS = 2 * SLOTS * BR + META
BELOW = Q * CB
HIGHEST = lax.Precision.HIGHEST
NB = 16
PIECE = 1
PIECES = BELOW // PIECE
ALL = ("z", "xc", "y")


def nt_dot(a, b, precision=None):
    return lax.dot_general(
        a, b, (((1,), (1,)), ((), ())), precision=precision, preferred_element_type=jnp.float32
    )


def pack_kernel(
    map_ref, order_ref, below_ref, desc_ref, head_ref, tail0_ref, tail1_ref,
    stage, meta, inverse, used, codes, in_sems, head_sem, tail_sem, meta_sem,
):
    count = map_ref.shape[1]
    parts = in_sems.shape[0]
    step = count // parts

    def load(k):
        part = pl.ds(k * step, step)
        return pltpu.make_async_copy(desc_ref.at[part], stage.at[part], in_sems.at[k])

    for k in range(parts):
        load(k).start()

    def clear(a, carry):
        inverse[order_ref[a]] = a
        used[a] = 0
        for s in range(SLOTS):
            codes[(a * SLOTS + s) * 4] = NONE
            codes[(a * SLOTS + s) * 4 + 1] = 0
            codes[(a * SLOTS + s) * 4 + 2] = 0
        return carry

    lax.fori_loop(0, NA, clear, 0)

    def route(d, carry):
        head = map_ref[0, d]
        a = inverse[head // CB]
        s = used[a]
        used[a] = s + 1
        dest = (a % XC) * Y + (a // XC) % Y
        i = jnp.bitwise_xor(a // (XC * Y), a % 2)
        slot = (dest * 2 + i) * SLOTS + s
        first, second = map_ref[1, d], map_ref[2, d]
        j1, j2 = jnp.int32(0), jnp.int32(0)
        for j in range(Q):
            g = below_ref[j, a]
            j1 = jnp.where(g == first, j, j1)
            j2 = jnp.where(g == second, j, j2)
        codes[slot * 4] = head % CB
        codes[slot * 4 + 1] = j1
        codes[slot * 4 + 2] = j2
        pltpu.make_async_copy(
            stage.at[d, pl.ds(0, BR)],
            head_ref.at[dest, pl.ds(pl.multiple_of((i * SLOTS + s) * BR, BR), BR)],
            head_sem,
        ).start()
        for k, out in ((0, tail0_ref), (1, tail1_ref)):
            @pl.when(i == k)
            def _():
                pltpu.make_async_copy(
                    stage.at[d, pl.ds(BR, 2 * BR)], out.at[dest, s], tail_sem
                ).start()
        return carry

    for k in range(parts):
        load(k).wait()
        lax.fori_loop(k * step, (k + 1) * step, route, 0)

    lane = lax.broadcasted_iota(jnp.int32, (META, 128), 1)

    def describe(dest, carry):
        row = jnp.zeros((META, 128), jnp.int32)
        for t in range(2 * SLOTS):
            for f in range(3):
                row = jnp.where(lane == t * 3 + f, codes[(dest * 2 * SLOTS + t) * 4 + f], row)
        meta[dest] = row.astype(jnp.float32).astype(jnp.bfloat16)
        return carry

    lax.fori_loop(0, PLANE, describe, 0)

    heads = stage.at[:, pl.ds(0, BR)]
    pltpu.make_async_copy(heads, heads, head_sem).wait()
    described = pltpu.make_async_copy(
        meta, head_ref.at[:, pl.ds(2 * SLOTS * BR, META)], meta_sem
    )
    described.start()
    tails = stage.at[:, pl.ds(BR, 2 * BR)]
    pltpu.make_async_copy(tails, tails, tail_sem).wait()
    described.wait()


def pack(row_map, anc_order, anc_below, desc_panel):
    smem = pl.BlockSpec(memory_space=pltpu.SMEM)
    hbm = pl.BlockSpec(memory_space=pltpu.HBM)
    dt = desc_panel.dtype
    return pl.pallas_call(
        pack_kernel,
        out_shape=(
            jax.ShapeDtypeStruct((PLANE, HEAD_ROWS, BR), dt),
            jax.ShapeDtypeStruct((PLANE, SLOTS, 2 * BR, BR), dt),
            jax.ShapeDtypeStruct((PLANE, SLOTS, 2 * BR, BR), dt),
        ),
        in_specs=[smem, smem, smem, hbm],
        out_specs=(hbm, hbm, hbm),
        scratch_shapes=[
            pltpu.VMEM(desc_panel.shape, dt),
            pltpu.VMEM((PLANE, META, BR), dt),
            pltpu.SMEM((NA,), jnp.int32),
            pltpu.SMEM((NA,), jnp.int32),
            pltpu.SMEM((NA * SLOTS * 4,), jnp.int32),
            pltpu.SemaphoreType.DMA((4,)),
            pltpu.SemaphoreType.DMA,
            pltpu.SemaphoreType.DMA,
            pltpu.SemaphoreType.DMA,
        ],
        name="pack",
    )(row_map.T, anc_order, anc_below.T, desc_panel)


GROUP = 8


def diag_kernel(codes, head_ref, out_ref):
    step = pl.program_id(0)

    @pl.when(step == 0)
    def _():
        out_ref[...] = jnp.zeros_like(out_ref)

    for g in range(GROUP):
        blocks = [head_ref[g, t * BR:(t + 1) * BR, :] for t in range(2 * SLOTS)]
        products = [nt_dot(block, block) for block in blocks]
        for t, product in enumerate(products):
            c = codes[step * GROUP + g, t * 3]
            place = jnp.where(c < CB, (t // SLOTS) * CB + c, 2 * CB)
            out_ref[place] = out_ref[place] + product


def diag_sums(codes, head):
    return pl.pallas_call(
        diag_kernel,
        out_shape=jax.ShapeDtypeStruct((2 * CB + 1, BR, BR), jnp.float32),
        grid_spec=pltpu.PrefetchScalarGridSpec(
            num_scalar_prefetch=1,
            grid=(PLANE // GROUP,),
            in_specs=[pl.BlockSpec((GROUP, HEAD_ROWS, BR), lambda k, codes: (k, 0, 0))],
            out_specs=pl.BlockSpec((2 * CB + 1, BR, BR), lambda k, codes: (0, 0, 0)),
        ),
        name="diag_sums",
    )(codes, head)


def below_kernel(i, codes, head_ref, tail_ref, out_ref):
    step = pl.program_id(0)

    @pl.when(step == 0)
    def _():
        out_ref[...] = jnp.zeros_like(out_ref)

    for g in range(GROUP):
        products = [
            nt_dot(tail_ref[g, s], head_ref[g, s * BR:(s + 1) * BR, :]) for s in range(SLOTS)
        ]
        for s, product in enumerate(products):
            t = i * SLOTS + s
            c = codes[step * GROUP + g, t * 3]
            for r in range(2):
                j = codes[step * GROUP + g, t * 3 + 1 + r]
                place = ((j % Y) * (Q // Y) + j // Y) * CB + c
                place = jnp.where(c < CB, place, BELOW)
                out_ref[place] = out_ref[place] + product[r * BR:(r + 1) * BR]


def below_sums(i, codes, head, tail):
    return pl.pallas_call(
        functools.partial(below_kernel, i),
        out_shape=jax.ShapeDtypeStruct((BELOW + PIECE, BR, BR), jnp.float32),
        grid_spec=pltpu.PrefetchScalarGridSpec(
            num_scalar_prefetch=1,
            grid=(PLANE // GROUP,),
            in_specs=[
                pl.BlockSpec((GROUP, SLOTS * BR, BR), lambda k, codes: (k, i, 0)),
                pl.BlockSpec((GROUP, SLOTS, 2 * BR, BR), lambda k, codes: (k, 0, 0, 0)),
            ],
            out_specs=pl.BlockSpec((BELOW + PIECE, BR, BR), lambda k, codes: (0, 0, 0)),
        ),
    )(codes, head, tail)


def nn_dot(a, b):
    return lax.dot_general(
        a, b, (((1,), (0,)), ((), ())), precision=HIGHEST, preferred_element_type=jnp.float32
    )


def tn_dot(a, b):
    return lax.dot_general(
        a, b, (((0,), (0,)), ((), ())), precision=HIGHEST, preferred_element_type=jnp.float32
    )


def factor_block(pair, between):
    sub = lax.broadcasted_iota(jnp.int32, (NB, BR), 0)
    sub2 = lax.broadcasted_iota(jnp.int32, (NB, 2 * BR), 0)
    lane = lax.broadcasted_iota(jnp.int32, (NB, BR), 1)
    for k in range(BR // NB):
        between(k)
        rows = pair[k * NB:(k + 1) * NB, :]
        cols = [jnp.broadcast_to(rows[:, k * NB + j:k * NB + j + 1], (NB, BR)) for j in range(NB)]
        for j in range(NB):
            scale = lax.rsqrt(cols[j][j:j + 1, :])
            column = cols[j] * scale
            below = jnp.where(sub > j, column, 0.0)
            row = rows[j:j + 1, :] * jnp.concatenate([scale, scale], axis=1)
            rows = jnp.where(sub2 == j, row, rows - jnp.concatenate([below, below], axis=1) * row)
            for m in range(j + 1, NB):
                cols[m] = cols[m] - below * column[m:m + 1, :]
        pair[k * NB:(k + 1) * NB, :] = rows
        start = (k + 1) * NB
        if start < BR:
            left = jnp.where(lane >= start, rows[:, :BR], 0.0)
            pair[start:, :] = pair[start:, :] - tn_dot(left, rows)[start:]


def factor_whole(lower_ref, inverse_ref, work, pair, between):
    width = work.shape[0]
    inverse_ref[...] = jnp.zeros_like(inverse_ref)
    row = lax.broadcasted_iota(jnp.int32, (BR, BR), 0)
    col = lax.broadcasted_iota(jnp.int32, (BR, BR), 1)
    all_rows = lax.broadcasted_iota(jnp.int32, (width, BR), 0)
    wide = lax.broadcasted_iota(jnp.int32, (BR, width), 1)
    high = lax.broadcasted_iota(jnp.int32, (BR, width), 0)

    def step(kb, carry):
        at = pl.ds(pl.multiple_of(kb * BR, BR), BR)
        pair[:, :BR] = work[at, at]
        pair[:, BR:] = jnp.where(row == col, 1.0, 0.0)
        factor_block(pair, functools.partial(between, kb))
        diagonal = jnp.where(col >= row, pair[:, :BR], 0.0).T
        small = jnp.where(col <= row, pair[:, BR:], 0.0)
        between(kb, BR // NB)
        panel = nt_dot(work[:, at], small, HIGHEST)
        panel = jnp.where(all_rows >= (kb + 1) * BR, panel, 0.0)
        lower_ref[:, at] = panel
        lower_ref[at, at] = diagonal
        work[...] = work[...] - nt_dot(panel, panel, HIGHEST)
        between(kb, BR // NB + 1)
        before = jnp.where(wide < kb * BR, lower_ref[at, :], 0.0)
        target = jnp.where(wide == high + kb * BR, 1.0, 0.0) - nn_dot(before, inverse_ref[...])
        inverse_ref[at, :] = nn_dot(small, target)
        return carry

    lax.fori_loop(0, width // BR, step, 0)


def remote(src, dst, send_sem, recv_sem, **device):
    return pltpu.make_async_remote_copy(
        src_ref=src, dst_ref=dst, send_sem=send_sem, recv_sem=recv_sem,
        device_id=device, device_id_type=pl.DeviceIdType.MESH,
    )


def signal(semaphore, **device):
    pl.semaphore_signal(
        semaphore, inc=1, device_id=device, device_id_type=pl.DeviceIdType.MESH
    )


def target_z(i, core, y):
    return y + Y * jnp.bitwise_xor(core, i)


def diag_reduce_kernel(sums, out, arrived, send_sems, recv_sems):
    z, y = lax.axis_index("z"), lax.axis_index("y")
    core = lax.axis_index("xc") % 2
    here = z % Y == y

    barrier = pltpu.get_barrier_semaphore()
    for source in range(Z):
        @pl.when(jnp.logical_and(here, source != z))
        def _():
            signal(barrier, z=jnp.int32(source))
    pl.semaphore_wait(barrier, 2 - here.astype(jnp.int32))

    def send(i):
        return remote(
            sums.at[pl.ds(i * CB, CB)], arrived.at[z], send_sems.at[i], recv_sems.at[z],
            z=target_z(i, core, y),
        )

    for i in range(2):
        @pl.when(target_z(i, core, y) != z)
        def _():
            send(i).start()

        @pl.when(target_z(i, core, y) == z)
        def _():
            arrived[z] = sums[i * CB:(i + 1) * CB]

    @pl.when(here)
    def _():
        for source in range(Z):
            @pl.when(source != z)
            def _():
                remote(
                    sums.at[pl.ds(0, CB)], arrived.at[source], send_sems.at[0],
                    recv_sems.at[source], z=(z + 1) % Z,
                ).wait_recv()
        update = arrived[0]
        for source in range(1, Z):
            update = update + arrived[source]
        out[...] = update

    @pl.when(jnp.logical_not(here))
    def _():
        out[...] = jnp.zeros_like(out)

    for i in range(2):
        @pl.when(target_z(i, core, y) != z)
        def _():
            send(i).wait_send()


def diag_reduce(sums):
    return pl.pallas_call(
        diag_reduce_kernel,
        out_shape=jax.ShapeDtypeStruct((CB, BR, BR), jnp.float32),
        in_specs=[IN_VMEM],
        out_specs=IN_VMEM,
        scratch_shapes=[
            pltpu.VMEM((Z, CB, BR, BR), jnp.float32),
            pltpu.SemaphoreType.DMA((2,)),
            pltpu.SemaphoreType.DMA((Z,)),
        ],
        compiler_params=pltpu.CompilerParams(collective_id=0, has_side_effects=True),
        name="diag_reduce",
    )(sums)


def spread_route(k):
    pairs = []
    for z in range(Z):
        for xc in range(XC):
            base = (z * XC + xc) * Y
            pairs.append((base + z % Y, base + (z + k) % Y))
    return pairs


class Chain:
    def __init__(self, i, sums, up, down, up_sems, down_sems, send_sem):
        self.z, self.y = lax.axis_index("z"), lax.axis_index("y")
        self.distance = (target_z(i, lax.axis_index("xc") % 2, self.y) - self.z + Z) % Z
        self.above, self.under = (self.z + 1) % Z, (self.z + Z - 1) % Z
        self.sums, self.up, self.down = sums, up, down
        self.up_sems, self.down_sems, self.send_sem = up_sems, down_sems, send_sem

    def meet(self, barrier):
        signal(barrier, z=self.above)
        signal(barrier, z=self.under)

    def copy(self, source, buffer, sems, q, to):
        return remote(source.at[q], buffer.at[q], self.send_sem, sems.at[q], z=to)

    def begin(self):
        for distance, buffer, sems, to in (
            (4, self.up, self.up_sems, self.above), (5, self.down, self.down_sems, self.under)
        ):
            @pl.when(self.distance == distance)
            def _():
                def body(q, carry):
                    self.copy(self.sums, buffer, sems, q, to).start()
                    return carry

                lax.fori_loop(0, PIECES, body, 0)

    def advance(self, q, deliver):
        for some, buffer, sems, to in (
            (jnp.logical_and(self.distance >= 1, self.distance <= 3),
             self.up, self.up_sems, self.above),
            (self.distance >= 6, self.down, self.down_sems, self.under),
        ):
            @pl.when(some)
            def _():
                self.copy(self.sums, buffer, sems, q, to).wait_recv()
                buffer[q] = buffer[q] + self.sums[q]
                self.copy(buffer, buffer, sems, q, to).start()

        @pl.when(self.distance == 0)
        def _():
            self.copy(self.sums, self.up, self.up_sems, q, self.above).wait_recv()
            self.copy(self.sums, self.down, self.down_sems, q, self.above).wait_recv()
            deliver(q, self.up[q] + self.down[q] + self.sums[q])

    def finish(self):
        @pl.when(self.distance != 0)
        def _():
            remote(self.up, self.up, self.send_sem, self.up_sems.at[0], z=self.above).wait_send()


CHAIN_SCRATCH = [
    pltpu.VMEM((PIECES, PIECE, BR, BR), jnp.float32),
    pltpu.VMEM((PIECES, PIECE, BR, BR), jnp.float32),
    pltpu.SemaphoreType.DMA((PIECES,)),
    pltpu.SemaphoreType.DMA((PIECES,)),
    pltpu.SemaphoreType.DMA,
]
IN_VMEM = pl.BlockSpec(memory_space=pltpu.VMEM)


def first_kernel(sums, total, up, down, up_sems, down_sems, send_sem):
    chain = Chain(0, sums, up, down, up_sems, down_sems, send_sem)
    barrier = pltpu.get_barrier_semaphore()
    chain.meet(barrier)
    pl.semaphore_wait(barrier, 2)
    chain.begin()

    def deliver(q, value):
        total[q] = value

    def body(q, carry):
        chain.advance(q, deliver)
        return carry

    lax.fori_loop(0, PIECES, body, 0)
    chain.finish()


def first_reduce(sums):
    return pl.pallas_call(
        first_kernel,
        out_shape=jax.ShapeDtypeStruct((PIECES, PIECE, BR, BR), jnp.float32),
        in_specs=[IN_VMEM],
        out_specs=IN_VMEM,
        scratch_shapes=CHAIN_SCRATCH,
        compiler_params=pltpu.CompilerParams(collective_id=1, has_side_effects=True),
        name="first_reduce",
    )(sums.reshape(PIECES + 1, PIECE, BR, BR))


def second_kernel(
    sums, total, strip, strip1, strip2, strip3, part, part1, part2, part3, out, lower, inverse,
    up, down, up_sems, down_sems, send_sem, final, final_sems, spread_sem, work, pair, strips,
):
    chain = Chain(1, sums, up, down, up_sems, down_sems, send_sem)
    z, y = chain.z, chain.y
    has_first = chain.distance == 4
    own = PIECES // Y
    barrier = pltpu.get_barrier_semaphore()
    chain.meet(barrier)
    for k in range(1, Y):
        signal(barrier, y=(y + k) % Y)
    pl.semaphore_wait(barrier, Y + 1)
    chain.begin()

    def spread(source, q):
        return remote(source.at[q], final.at[q % own], spread_sem, final_sems.at[q % own], y=q // own)

    @pl.when(has_first)
    def _():
        def body(q, carry):
            @pl.when(q // own == y)
            def _():
                out[q % own] = total[q]

            @pl.when(q // own != y)
            def _():
                spread(total, q).start()

            return carry

        lax.fori_loop(0, PIECES, body, 0)

    def deliver(q, value):
        @pl.when(q // own == y)
        def _():
            out[q % own] = value

        @pl.when(q // own != y)
        def _():
            up[q] = value
            spread(up, q).start()

    for k, one in enumerate((strip, strip1, strip2, strip3)):
        strips[(y + Y - k) % Y] = one[...]
    work[...] = jnp.zeros_like(work)
    blocks = {(1, 0): strips[1, 0], (2, 1): strips[2, 0], (3, 2): strips[3, 0],
              (3, 0): strips[0, 0].T, (2, 0): strips[2, 1], (3, 1): strips[3, 1]}
    for c in range(CB):
        blocks[c, c] = strips[c, 2] - (part[c] + part1[c] + part2[c] + part3[c])
    for (b, c), block in blocks.items():
        work[b * BR:(b + 1) * BR, c * BR:(c + 1) * BR] = block

    turns = (2, 1, 1, 2, 1, 1, 1, 1, 2, 2)

    def between(kb, k):
        for n in range(turns[k]):
            q = kb * sum(turns) + sum(turns[:k]) + n

            @pl.when(q < PIECES)
            def _():
                chain.advance(q, deliver)

    factor_whole(lower, inverse, work, pair, between)
    chain.finish()

    @pl.when(z % Y == y)
    def _():
        part = up.at[pl.ds(0, PIECES - own)]
        remote(part, part, spread_sem, up_sems.at[0], z=chain.above).wait_send()

    @pl.when(z % Y != y)
    def _():
        def body(place, carry):
            chain.copy(sums, final, final_sems, place, chain.above).wait_recv()
            out[place] = final[place]
            return carry

        lax.fori_loop(0, own, body, 0)


def second_reduce(sums, total, strips, parts):
    own, width = PIECES // Y, CB * BR
    square = jax.ShapeDtypeStruct((width, width), jnp.float32)
    return pl.pallas_call(
        second_kernel,
        out_shape=(jax.ShapeDtypeStruct((own, PIECE, BR, BR), jnp.float32), square, square),
        in_specs=[IN_VMEM] * (2 + 2 * Y),
        out_specs=(IN_VMEM,) * 3,
        scratch_shapes=CHAIN_SCRATCH + [
            pltpu.VMEM((own, PIECE, BR, BR), jnp.float32),
            pltpu.SemaphoreType.DMA((own,)),
            pltpu.SemaphoreType.DMA,
            pltpu.VMEM((width, width), jnp.float32),
            pltpu.VMEM((BR, 2 * BR), jnp.float32),
            pltpu.VMEM((Y, 3, BR, BR), jnp.float32),
        ],
        compiler_params=pltpu.CompilerParams(collective_id=2, has_side_effects=True),
        name="second_reduce",
    )(sums.reshape(PIECES + 1, PIECE, BR, BR), total, *strips, *parts)


def solve_kernel(y_ref, rows_ref, lower_ref, inverse_ref, update_ref, out_ref):
    m = pl.program_id(0)

    @pl.when(m == 0)
    def _():
        out_ref[0, 0, 0] = lower_ref[...]

    @pl.when(m > 0)
    def _():
        update = jnp.concatenate([update_ref[0, c] for c in range(CB)], axis=1)
        out_ref[0, 0, 0] = nt_dot(rows_ref[0, 0, 0] - update, inverse_ref[...], HIGHEST)


def solve(anc_panel, lower, inverse, update, y):
    width = anc_panel.shape[4]
    update = update.reshape(Q // Y, CB, BR, BR)
    return pl.pallas_call(
        solve_kernel,
        out_shape=jax.ShapeDtypeStruct(anc_panel.shape, jnp.float32),
        grid_spec=pltpu.PrefetchScalarGridSpec(
            num_scalar_prefetch=1,
            grid=(anc_panel.shape[1],),
            in_specs=[
                pl.BlockSpec((1, 1, 1, BR, width), lambda m, y: (0, m, 0, 0, 0)),
                pl.BlockSpec((BR, width), lambda m, y: (y[0], 0)),
                pl.BlockSpec((width, width), lambda m, y: (0, 0)),
                pl.BlockSpec((1, CB, BR, BR), lambda m, y: (jnp.maximum(m - 1, 0), 0, 0, 0)),
            ],
            out_specs=pl.BlockSpec((1, 1, 1, BR, width), lambda m, y: (0, m, 0, 0, 0)),
        ),
        name="solve",
    )(y, anc_panel, lower, inverse, update)


def exchange(value):
    return lax.all_to_all(value, ("xc", "y"), split_axis=0, concat_axis=0, tiled=True)


def strip_blocks(anc_panel, y):
    strip = anc_panel[0, 0, 0]
    columns = [lax.rem(y + Y - 1, Y), lax.rem(y + 2, Y), y]
    zero = jnp.int32(0)
    return jnp.stack(
        [lax.dynamic_slice(strip, (zero, c * BR), (BR, BR), allow_negative_indices=False) for c in columns]
    )


def shards(desc_panel, row_map, anc_order, anc_below, anc_panel):
    y = lax.axis_index("y").astype(jnp.int32)
    head, tail0, tail1 = pack(row_map, anc_order, anc_below, desc_panel)
    head = exchange(head)
    tail0, head, anc_panel = lax.optimization_barrier((tail0, head, anc_panel))
    tail0 = exchange(tail0)
    codes = head[:, 2 * SLOTS * BR, : 2 * SLOTS * 3].astype(jnp.int32)
    part = diag_reduce(diag_sums(codes, head))
    strip = strip_blocks(anc_panel, y)
    strips, parts = [strip], [part]
    for k in range(1, Y):
        strips.append(lax.ppermute(strip, "y", [(b, (b + k) % Y) for b in range(Y)]))
    for k in range(1, Y):
        parts.append(lax.ppermute(part, ALL, spread_route(k)))
    tail1, tail0, part = lax.optimization_barrier((tail1, tail0, part))
    tail1 = exchange(tail1)
    total = first_reduce(below_sums(0, codes, head, tail0))
    tail1, total = lax.optimization_barrier((tail1, total))
    sums = below_sums(1, codes, head, tail1)
    update, lower, inverse = second_reduce(sums, total, strips, parts)
    return solve(anc_panel, lower, inverse, update, y.reshape(1))


def solution(mesh):
    grid = Mesh(mesh.devices.reshape(Z, XC, Y), ALL)
    in_specs = (
        P(ALL, None, None),
        P(ALL, None),
        P(),
        P(),
        P(("z", "xc"), None, "y", None, None),
    )
    out_specs = P(("z", "xc"), None, "y", None, None)
    return jax.shard_map(
        shards, mesh=grid, in_specs=in_specs, out_specs=out_specs, check_vma=False
    )
```

```python
import functools

import jax
import jax.numpy as jnp
from jax import lax
from jax.experimental import pallas as pl
from jax.experimental.pallas import tpu as pltpu
from jax.sharding import Mesh
from jax.sharding import PartitionSpec as P

Z, XC, Y = 8, 8, 4
PLANE = XC * Y
BR = 128
CB = 4
Q = 12
SLOTS = 2
NA = 64
NONE = 7
META = 16
HEAD_ROWS = 2 * SLOTS * BR + META
BELOW = Q * CB
HIGHEST = lax.Precision.HIGHEST
NB = 16
PIECE = 1
PIECES = BELOW // PIECE
ALL = ("z", "xc", "y")


def nt_dot(a, b, precision=None):
    return lax.dot_general(
        a, b, (((1,), (1,)), ((), ())), precision=precision, preferred_element_type=jnp.float32
    )


def pack_kernel(
    map_ref, order_ref, below_ref, desc_ref, head_ref, tail0_ref, tail1_ref,
    stage, meta, inverse, used, codes, in_sems, head_sem, tail_sem, meta_sem,
):
    count = map_ref.shape[1]
    parts = in_sems.shape[0]
    step = count // parts

    def load(k):
        part = pl.ds(k * step, step)
        return pltpu.make_async_copy(desc_ref.at[part], stage.at[part], in_sems.at[k])

    for k in range(parts):
        load(k).start()

    def clear(a, carry):
        inverse[order_ref[a]] = a
        used[a] = 0
        for s in range(SLOTS):
            codes[(a * SLOTS + s) * 4] = NONE
            codes[(a * SLOTS + s) * 4 + 1] = 0
            codes[(a * SLOTS + s) * 4 + 2] = 0
        return carry

    lax.fori_loop(0, NA, clear, 0)

    def route(d, carry):
        head = map_ref[0, d]
        a = inverse[head // CB]
        s = used[a]
        used[a] = s + 1
        i = jnp.bitwise_xor(a // (XC * Y), a % 2)
        dest = (a % XC) * Y + (a // XC + 2 * i) % Y
        slot = (dest * 2 + i) * SLOTS + s
        first, second = map_ref[1, d], map_ref[2, d]
        j1, j2 = jnp.int32(0), jnp.int32(0)
        for j in range(Q):
            g = below_ref[j, a]
            j1 = jnp.where(g == first, j, j1)
            j2 = jnp.where(g == second, j, j2)
        codes[slot * 4] = head % CB
        codes[slot * 4 + 1] = j1
        codes[slot * 4 + 2] = j2
        pltpu.make_async_copy(
            stage.at[d, pl.ds(0, BR)],
            head_ref.at[dest, pl.ds(pl.multiple_of((i * SLOTS + s) * BR, BR), BR)],
            head_sem,
        ).start()
        for k, out in ((0, tail0_ref), (1, tail1_ref)):
            @pl.when(i == k)
            def _():
                pltpu.make_async_copy(
                    stage.at[d, pl.ds(BR, 2 * BR)], out.at[dest, s], tail_sem
                ).start()
        return carry

    for k in range(parts):
        load(k).wait()
        lax.fori_loop(k * step, (k + 1) * step, route, 0)

    lane = lax.broadcasted_iota(jnp.int32, (META, 128), 1)

    def describe(dest, carry):
        row = jnp.zeros((META, 128), jnp.int32)
        for t in range(2 * SLOTS):
            for f in range(3):
                row = jnp.where(lane == t * 3 + f, codes[(dest * 2 * SLOTS + t) * 4 + f], row)
        meta[dest] = row.astype(jnp.float32).astype(jnp.bfloat16)
        return carry

    lax.fori_loop(0, PLANE, describe, 0)

    heads = stage.at[:, pl.ds(0, BR)]
    pltpu.make_async_copy(heads, heads, head_sem).wait()
    described = pltpu.make_async_copy(
        meta, head_ref.at[:, pl.ds(2 * SLOTS * BR, META)], meta_sem
    )
    described.start()
    tails = stage.at[:, pl.ds(BR, 2 * BR)]
    pltpu.make_async_copy(tails, tails, tail_sem).wait()
    described.wait()


def pack(row_map, anc_order, anc_below, desc_panel):
    smem = pl.BlockSpec(memory_space=pltpu.SMEM)
    hbm = pl.BlockSpec(memory_space=pltpu.HBM)
    dt = desc_panel.dtype
    return pl.pallas_call(
        pack_kernel,
        out_shape=(
            jax.ShapeDtypeStruct((PLANE, HEAD_ROWS, BR), dt),
            jax.ShapeDtypeStruct((PLANE, SLOTS, 2 * BR, BR), dt),
            jax.ShapeDtypeStruct((PLANE, SLOTS, 2 * BR, BR), dt),
        ),
        in_specs=[smem, smem, smem, hbm],
        out_specs=(hbm, hbm, hbm),
        scratch_shapes=[
            pltpu.VMEM(desc_panel.shape, dt),
            pltpu.VMEM((PLANE, META, BR), dt),
            pltpu.SMEM((NA,), jnp.int32),
            pltpu.SMEM((NA,), jnp.int32),
            pltpu.SMEM((NA * SLOTS * 4,), jnp.int32),
            pltpu.SemaphoreType.DMA((4,)),
            pltpu.SemaphoreType.DMA,
            pltpu.SemaphoreType.DMA,
            pltpu.SemaphoreType.DMA,
        ],
        name="pack",
    )(row_map.T, anc_order, anc_below.T, desc_panel)


GROUP = 8


def diag_kernel(codes, head_ref, out_ref):
    step = pl.program_id(0)

    @pl.when(step == 0)
    def _():
        out_ref[...] = jnp.zeros_like(out_ref)

    for g in range(GROUP):
        blocks = [head_ref[g, t * BR:(t + 1) * BR, :] for t in range(2 * SLOTS)]
        products = [nt_dot(block, block) for block in blocks]
        for t, product in enumerate(products):
            c = codes[step * GROUP + g, t * 3]
            place = jnp.where(c < CB, (t // SLOTS) * CB + c, 2 * CB)
            out_ref[place] = out_ref[place] + product


def diag_sums(codes, head):
    return pl.pallas_call(
        diag_kernel,
        out_shape=jax.ShapeDtypeStruct((2 * CB + 1, BR, BR), jnp.float32),
        grid_spec=pltpu.PrefetchScalarGridSpec(
            num_scalar_prefetch=1,
            grid=(PLANE // GROUP,),
            in_specs=[pl.BlockSpec((GROUP, HEAD_ROWS, BR), lambda k, codes: (k, 0, 0))],
            out_specs=pl.BlockSpec((2 * CB + 1, BR, BR), lambda k, codes: (0, 0, 0)),
        ),
        name="diag_sums",
    )(codes, head)


def below_kernel(i, codes, head_ref, tail_ref, out_ref):
    step = pl.program_id(0)

    @pl.when(step == 0)
    def _():
        out_ref[...] = jnp.zeros_like(out_ref)

    for g in range(GROUP):
        products = [
            nt_dot(tail_ref[g, s], head_ref[g, s * BR:(s + 1) * BR, :]) for s in range(SLOTS)
        ]
        for s, product in enumerate(products):
            t = i * SLOTS + s
            c = codes[step * GROUP + g, t * 3]
            for r in range(2):
                j = codes[step * GROUP + g, t * 3 + 1 + r]
                place = ((j % Y) * (Q // Y) + j // Y) * CB + c
                place = jnp.where(c < CB, place, BELOW)
                out_ref[place] = out_ref[place] + product[r * BR:(r + 1) * BR]


def below_sums(i, codes, head, tail):
    return pl.pallas_call(
        functools.partial(below_kernel, i),
        out_shape=jax.ShapeDtypeStruct((BELOW + PIECE, BR, BR), jnp.float32),
        grid_spec=pltpu.PrefetchScalarGridSpec(
            num_scalar_prefetch=1,
            grid=(PLANE // GROUP,),
            in_specs=[
                pl.BlockSpec((GROUP, SLOTS * BR, BR), lambda k, codes: (k, i, 0)),
                pl.BlockSpec((GROUP, SLOTS, 2 * BR, BR), lambda k, codes: (k, 0, 0, 0)),
            ],
            out_specs=pl.BlockSpec((BELOW + PIECE, BR, BR), lambda k, codes: (0, 0, 0)),
        ),
    )(codes, head, tail)


def nn_dot(a, b):
    return lax.dot_general(
        a, b, (((1,), (0,)), ((), ())), precision=HIGHEST, preferred_element_type=jnp.float32
    )


def tn_dot(a, b):
    return lax.dot_general(
        a, b, (((0,), (0,)), ((), ())), precision=HIGHEST, preferred_element_type=jnp.float32
    )


def factor_block(pair, between):
    sub = lax.broadcasted_iota(jnp.int32, (NB, BR), 0)
    sub2 = lax.broadcasted_iota(jnp.int32, (NB, 2 * BR), 0)
    lane = lax.broadcasted_iota(jnp.int32, (NB, BR), 1)
    for k in range(BR // NB):
        between(k)
        rows = pair[k * NB:(k + 1) * NB, :]
        cols = [jnp.broadcast_to(rows[:, k * NB + j:k * NB + j + 1], (NB, BR)) for j in range(NB)]
        for j in range(NB):
            scale = lax.rsqrt(cols[j][j:j + 1, :])
            column = cols[j] * scale
            below = jnp.where(sub > j, column, 0.0)
            row = rows[j:j + 1, :] * jnp.concatenate([scale, scale], axis=1)
            rows = jnp.where(sub2 == j, row, rows - jnp.concatenate([below, below], axis=1) * row)
            for m in range(j + 1, NB):
                cols[m] = cols[m] - below * column[m:m + 1, :]
        pair[k * NB:(k + 1) * NB, :] = rows
        start = (k + 1) * NB
        if start < BR:
            left = jnp.where(lane >= start, rows[:, :BR], 0.0)
            pair[start:, :] = pair[start:, :] - tn_dot(left, rows)[start:]


def factor_whole(lower_ref, inverse_ref, work, pair, between):
    width = work.shape[0]
    inverse_ref[...] = jnp.zeros_like(inverse_ref)
    row = lax.broadcasted_iota(jnp.int32, (BR, BR), 0)
    col = lax.broadcasted_iota(jnp.int32, (BR, BR), 1)
    all_rows = lax.broadcasted_iota(jnp.int32, (width, BR), 0)
    wide = lax.broadcasted_iota(jnp.int32, (BR, width), 1)
    high = lax.broadcasted_iota(jnp.int32, (BR, width), 0)

    def step(kb, carry):
        at = pl.ds(pl.multiple_of(kb * BR, BR), BR)
        pair[:, :BR] = work[at, at]
        pair[:, BR:] = jnp.where(row == col, 1.0, 0.0)
        factor_block(pair, functools.partial(between, kb))
        diagonal = jnp.where(col >= row, pair[:, :BR], 0.0).T
        small = jnp.where(col <= row, pair[:, BR:], 0.0)
        between(kb, BR // NB)
        panel = nt_dot(work[:, at], small, HIGHEST)
        panel = jnp.where(all_rows >= (kb + 1) * BR, panel, 0.0)
        lower_ref[:, at] = panel
        lower_ref[at, at] = diagonal
        work[...] = work[...] - nt_dot(panel, panel, HIGHEST)
        between(kb, BR // NB + 1)
        before = jnp.where(wide < kb * BR, lower_ref[at, :], 0.0)
        target = jnp.where(wide == high + kb * BR, 1.0, 0.0) - nn_dot(before, inverse_ref[...])
        inverse_ref[at, :] = nn_dot(small, target)
        return carry

    lax.fori_loop(0, width // BR, step, 0)


def remote(src, dst, send_sem, recv_sem, **device):
    return pltpu.make_async_remote_copy(
        src_ref=src, dst_ref=dst, send_sem=send_sem, recv_sem=recv_sem,
        device_id=device, device_id_type=pl.DeviceIdType.MESH,
    )


def signal(semaphore, **device):
    pl.semaphore_signal(
        semaphore, inc=1, device_id=device, device_id_type=pl.DeviceIdType.MESH
    )


def target_z(i, core, y):
    return (y + 2 * i) % Y + Y * jnp.bitwise_xor(core, i)


def gather_y(z, core):
    return (z + 2 * ((z // Y) ^ core)) % Y


def diag_reduce_kernel(sums, out, arrived, send_sems, recv_sems):
    z, y = lax.axis_index("z"), lax.axis_index("y")
    core = lax.axis_index("xc") % 2
    here = gather_y(z, core) == y

    barrier = pltpu.get_barrier_semaphore()
    for source in range(Z):
        @pl.when(jnp.logical_and(here, source != z))
        def _():
            signal(barrier, z=jnp.int32(source))
    pl.semaphore_wait(barrier, 2 - here.astype(jnp.int32))

    def send(i):
        return remote(
            sums.at[pl.ds(i * CB, CB)], arrived.at[z], send_sems.at[i], recv_sems.at[z],
            z=target_z(i, core, y),
        )

    for i in range(2):
        @pl.when(target_z(i, core, y) != z)
        def _():
            send(i).start()

        @pl.when(target_z(i, core, y) == z)
        def _():
            arrived[z] = sums[i * CB:(i + 1) * CB]

    @pl.when(here)
    def _():
        for source in range(Z):
            @pl.when(source != z)
            def _():
                remote(
                    sums.at[pl.ds(0, CB)], arrived.at[source], send_sems.at[0],
                    recv_sems.at[source], z=(z + 1) % Z,
                ).wait_recv()
        update = arrived[0]
        for source in range(1, Z):
            update = update + arrived[source]
        out[...] = update

    @pl.when(jnp.logical_not(here))
    def _():
        out[...] = jnp.zeros_like(out)

    for i in range(2):
        @pl.when(target_z(i, core, y) != z)
        def _():
            send(i).wait_send()


def diag_reduce(sums):
    return pl.pallas_call(
        diag_reduce_kernel,
        out_shape=jax.ShapeDtypeStruct((CB, BR, BR), jnp.float32),
        in_specs=[IN_VMEM],
        out_specs=IN_VMEM,
        scratch_shapes=[
            pltpu.VMEM((Z, CB, BR, BR), jnp.float32),
            pltpu.SemaphoreType.DMA((2,)),
            pltpu.SemaphoreType.DMA((Z,)),
        ],
        compiler_params=pltpu.CompilerParams(collective_id=0, has_side_effects=True),
        name="diag_reduce",
    )(sums)


def spread_route(k):
    pairs = []
    for z in range(Z):
        for xc in range(XC):
            base = (z * XC + xc) * Y
            row = gather_y(z, xc % 2)
            pairs.append((base + row, base + (row + k) % Y))
    return pairs


class Chain:
    def __init__(self, i, sums, up, down, up_sems, down_sems, send_sem):
        self.z, self.y = lax.axis_index("z"), lax.axis_index("y")
        self.distance = (target_z(i, lax.axis_index("xc") % 2, self.y) - self.z + Z) % Z
        self.above, self.under = (self.z + 1) % Z, (self.z + Z - 1) % Z
        self.sums, self.up, self.down = sums, up, down
        self.up_sems, self.down_sems, self.send_sem = up_sems, down_sems, send_sem

    def meet(self, barrier):
        signal(barrier, z=self.above)
        signal(barrier, z=self.under)

    def copy(self, source, buffer, sems, q, to):
        return remote(source.at[q], buffer.at[q], self.send_sem, sems.at[q], z=to)

    def begin(self):
        for distance, buffer, sems, to in (
            (4, self.up, self.up_sems, self.above), (5, self.down, self.down_sems, self.under)
        ):
            @pl.when(self.distance == distance)
            def _():
                def body(q, carry):
                    self.copy(self.sums, buffer, sems, q, to).start()
                    return carry

                lax.fori_loop(0, PIECES, body, 0)

    def advance(self, q, deliver):
        for some, buffer, sems, to in (
            (jnp.logical_and(self.distance >= 1, self.distance <= 3),
             self.up, self.up_sems, self.above),
            (self.distance >= 6, self.down, self.down_sems, self.under),
        ):
            @pl.when(some)
            def _():
                self.copy(self.sums, buffer, sems, q, to).wait_recv()
                buffer[q] = buffer[q] + self.sums[q]
                self.copy(buffer, buffer, sems, q, to).start()

        @pl.when(self.distance == 0)
        def _():
            self.copy(self.sums, self.up, self.up_sems, q, self.above).wait_recv()
            self.copy(self.sums, self.down, self.down_sems, q, self.above).wait_recv()
            deliver(q, self.up[q] + self.down[q] + self.sums[q])

    def finish(self):
        @pl.when(self.distance != 0)
        def _():
            remote(self.up, self.up, self.send_sem, self.up_sems.at[0], z=self.above).wait_send()


CHAIN_SCRATCH = [
    pltpu.VMEM((PIECES, PIECE, BR, BR), jnp.float32),
    pltpu.VMEM((PIECES, PIECE, BR, BR), jnp.float32),
    pltpu.SemaphoreType.DMA((PIECES,)),
    pltpu.SemaphoreType.DMA((PIECES,)),
    pltpu.SemaphoreType.DMA,
]
IN_VMEM = pl.BlockSpec(memory_space=pltpu.VMEM)


def first_kernel(sums, total, up, down, up_sems, down_sems, send_sem):
    chain = Chain(0, sums, up, down, up_sems, down_sems, send_sem)
    barrier = pltpu.get_barrier_semaphore()
    chain.meet(barrier)
    pl.semaphore_wait(barrier, 2)
    chain.begin()

    def deliver(q, value):
        total[q] = value

    def body(q, carry):
        chain.advance(q, deliver)
        return carry

    lax.fori_loop(0, PIECES, body, 0)
    chain.finish()


def first_reduce(sums):
    return pl.pallas_call(
        first_kernel,
        out_shape=jax.ShapeDtypeStruct((PIECES, PIECE, BR, BR), jnp.float32),
        in_specs=[IN_VMEM],
        out_specs=IN_VMEM,
        scratch_shapes=CHAIN_SCRATCH,
        compiler_params=pltpu.CompilerParams(collective_id=1, has_side_effects=True),
        name="first_reduce",
    )(sums.reshape(PIECES + 1, PIECE, BR, BR))


def second_kernel(
    sums, total, strip, strip1, strip2, strip3, part, part1, part2, part3, out, lower, inverse,
    up, down, up_sems, down_sems, send_sem, final, final_sems, spread_sem, work, pair, strips,
):
    chain = Chain(1, sums, up, down, up_sems, down_sems, send_sem)
    z, y = chain.z, chain.y
    core = lax.axis_index("xc") % 2
    here = gather_y(z, core) == y
    has_first = target_z(0, core, y) == z
    own = PIECES // Y
    barrier = pltpu.get_barrier_semaphore()
    chain.meet(barrier)
    for k in range(1, Y):
        signal(barrier, y=(y + k) % Y)
    pl.semaphore_wait(barrier, Y + 1)
    chain.begin()

    def spread(source, q):
        return remote(source.at[q], final.at[q % own], spread_sem, final_sems.at[q % own], y=q // own)

    @pl.when(has_first)
    def _():
        def body(q, carry):
            @pl.when(q // own == y)
            def _():
                out[q % own] = total[q]

            @pl.when(q // own != y)
            def _():
                spread(total, q).start()

            return carry

        lax.fori_loop(0, PIECES, body, 0)

    def deliver(q, value):
        @pl.when(q // own == y)
        def _():
            out[q % own] = value

        @pl.when(q // own != y)
        def _():
            up[q] = value
            spread(up, q).start()

    for k, one in enumerate((strip, strip1, strip2, strip3)):
        strips[(y + Y - k) % Y] = one[...]
    work[...] = jnp.zeros_like(work)
    blocks = {(1, 0): strips[1, 0], (2, 1): strips[2, 0], (3, 2): strips[3, 0],
              (3, 0): strips[0, 0].T, (2, 0): strips[2, 1], (3, 1): strips[3, 1]}
    for c in range(CB):
        blocks[c, c] = strips[c, 2] - (part[c] + part1[c] + part2[c] + part3[c])
    for (b, c), block in blocks.items():
        work[b * BR:(b + 1) * BR, c * BR:(c + 1) * BR] = block

    turns = (2, 1, 1, 2, 1, 1, 1, 1, 2, 2)

    def between(kb, k):
        for n in range(turns[k]):
            q = kb * sum(turns) + sum(turns[:k]) + n

            @pl.when(q < PIECES)
            def _():
                chain.advance(q, deliver)

    factor_whole(lower, inverse, work, pair, between)
    chain.finish()

    @pl.when(here)
    def _():
        part = up.at[pl.ds(0, PIECES - own)]
        remote(part, part, spread_sem, up_sems.at[0], z=chain.above).wait_send()

    @pl.when(jnp.logical_not(here))
    def _():
        def body(place, carry):
            chain.copy(sums, final, final_sems, place, chain.above).wait_recv()
            out[place] = final[place]
            return carry

        lax.fori_loop(0, own, body, 0)


def second_reduce(sums, total, strips, parts):
    own, width = PIECES // Y, CB * BR
    square = jax.ShapeDtypeStruct((width, width), jnp.float32)
    return pl.pallas_call(
        second_kernel,
        out_shape=(jax.ShapeDtypeStruct((own, PIECE, BR, BR), jnp.float32), square, square),
        in_specs=[IN_VMEM] * (2 + 2 * Y),
        out_specs=(IN_VMEM,) * 3,
        scratch_shapes=CHAIN_SCRATCH + [
            pltpu.VMEM((own, PIECE, BR, BR), jnp.float32),
            pltpu.SemaphoreType.DMA((own,)),
            pltpu.SemaphoreType.DMA,
            pltpu.VMEM((width, width), jnp.float32),
            pltpu.VMEM((BR, 2 * BR), jnp.float32),
            pltpu.VMEM((Y, 3, BR, BR), jnp.float32),
        ],
        compiler_params=pltpu.CompilerParams(collective_id=2, has_side_effects=True),
        name="second_reduce",
    )(sums.reshape(PIECES + 1, PIECE, BR, BR), total, *strips, *parts)


def solve_kernel(y_ref, rows_ref, lower_ref, inverse_ref, update_ref, out_ref):
    m = pl.program_id(0)

    @pl.when(m == 0)
    def _():
        out_ref[0, 0, 0] = lower_ref[...]

    @pl.when(m > 0)
    def _():
        update = jnp.concatenate([update_ref[0, c] for c in range(CB)], axis=1)
        out_ref[0, 0, 0] = nt_dot(rows_ref[0, 0, 0] - update, inverse_ref[...], HIGHEST)


def solve(anc_panel, lower, inverse, update, y):
    width = anc_panel.shape[4]
    update = update.reshape(Q // Y, CB, BR, BR)
    return pl.pallas_call(
        solve_kernel,
        out_shape=jax.ShapeDtypeStruct(anc_panel.shape, jnp.float32),
        grid_spec=pltpu.PrefetchScalarGridSpec(
            num_scalar_prefetch=1,
            grid=(anc_panel.shape[1],),
            in_specs=[
                pl.BlockSpec((1, 1, 1, BR, width), lambda m, y: (0, m, 0, 0, 0)),
                pl.BlockSpec((BR, width), lambda m, y: (y[0], 0)),
                pl.BlockSpec((width, width), lambda m, y: (0, 0)),
                pl.BlockSpec((1, CB, BR, BR), lambda m, y: (jnp.maximum(m - 1, 0), 0, 0, 0)),
            ],
            out_specs=pl.BlockSpec((1, 1, 1, BR, width), lambda m, y: (0, m, 0, 0, 0)),
        ),
        name="solve",
    )(y, anc_panel, lower, inverse, update)


def exchange(value):
    return lax.all_to_all(value, ("xc", "y"), split_axis=0, concat_axis=0, tiled=True)


def strip_blocks(anc_panel, y):
    strip = anc_panel[0, 0, 0]
    columns = [lax.rem(y + Y - 1, Y), lax.rem(y + 2, Y), y]
    zero = jnp.int32(0)
    return jnp.stack(
        [lax.dynamic_slice(strip, (zero, c * BR), (BR, BR), allow_negative_indices=False) for c in columns]
    )


def shards(desc_panel, row_map, anc_order, anc_below, anc_panel):
    y = lax.axis_index("y").astype(jnp.int32)
    head, tail0, tail1 = pack(row_map, anc_order, anc_below, desc_panel)
    head = exchange(head)
    tail0, head, anc_panel = lax.optimization_barrier((tail0, head, anc_panel))
    tail0 = exchange(tail0)
    codes = head[:, 2 * SLOTS * BR, : 2 * SLOTS * 3].astype(jnp.int32)
    part = diag_reduce(diag_sums(codes, head))
    strip = strip_blocks(anc_panel, y)
    strips, parts = [strip], [part]
    for k in range(1, Y):
        strips.append(lax.ppermute(strip, "y", [(b, (b + k) % Y) for b in range(Y)]))
    for k in range(1, Y):
        parts.append(lax.ppermute(part, ALL, spread_route(k)))
    tail1, tail0, part = lax.optimization_barrier((tail1, tail0, part))
    tail1 = exchange(tail1)
    total = first_reduce(below_sums(0, codes, head, tail0))
    tail1, total = lax.optimization_barrier((tail1, total))
    sums = below_sums(1, codes, head, tail1)
    update, lower, inverse = second_reduce(sums, total, strips, parts)
    return solve(anc_panel, lower, inverse, update, y.reshape(1))


def solution(mesh):
    grid = Mesh(mesh.devices.reshape(Z, XC, Y), ALL)
    in_specs = (
        P(ALL, None, None),
        P(ALL, None),
        P(),
        P(),
        P(("z", "xc"), None, "y", None, None),
    )
    out_specs = P(("z", "xc"), None, "y", None, None)
    return jax.shard_map(
        shards, mesh=grid, in_specs=in_specs, out_specs=out_specs, check_vma=False
    )
```

```python
import functools

import jax
import jax.numpy as jnp
from jax import lax
from jax.experimental import pallas as pl
from jax.experimental.pallas import tpu as pltpu
from jax.sharding import Mesh
from jax.sharding import PartitionSpec as P

Z, XC, Y = 8, 8, 4
PLANE = XC * Y
BR = 128
CB = 4
Q = 12
SLOTS = 2
NA = 64
NONE = 7
META = 16
HEAD_ROWS = 2 * SLOTS * BR + META
BELOW = Q * CB
HIGHEST = lax.Precision.HIGHEST
NB = 16
PIECE = 1
PIECES = BELOW // PIECE
ALL = ("z", "xc", "y")


def nt_dot(a, b, precision=None):
    return lax.dot_general(
        a, b, (((1,), (1,)), ((), ())), precision=precision, preferred_element_type=jnp.float32
    )


def pack_kernel(
    map_ref, order_ref, below_ref, desc_ref, head_ref, tail0_ref, tail1_ref,
    stage, meta, inverse, used, codes, in_sems, head_sem, tail_sem, meta_sem,
):
    count = map_ref.shape[1]
    parts = in_sems.shape[0]
    step = count // parts

    def load(k):
        part = pl.ds(k * step, step)
        return pltpu.make_async_copy(desc_ref.at[part], stage.at[part], in_sems.at[k])

    for k in range(parts):
        load(k).start()

    def clear(a, carry):
        inverse[order_ref[a]] = a
        used[a] = 0
        for s in range(SLOTS):
            codes[(a * SLOTS + s) * 4] = NONE
            codes[(a * SLOTS + s) * 4 + 1] = 0
            codes[(a * SLOTS + s) * 4 + 2] = 0
        return carry

    lax.fori_loop(0, NA, clear, 0)

    def route(d, carry):
        head = map_ref[0, d]
        a = inverse[head // CB]
        s = used[a]
        used[a] = s + 1
        dest = (a % XC) * Y + (a // XC) % Y
        i = jnp.bitwise_xor(a // (XC * Y), a % 2)
        slot = (dest * 2 + i) * SLOTS + s
        first, second = map_ref[1, d], map_ref[2, d]
        j1, j2 = jnp.int32(0), jnp.int32(0)
        for j in range(Q):
            g = below_ref[j, a]
            j1 = jnp.where(g == first, j, j1)
            j2 = jnp.where(g == second, j, j2)
        codes[slot * 4] = head % CB
        codes[slot * 4 + 1] = j1
        codes[slot * 4 + 2] = j2
        pltpu.make_async_copy(
            stage.at[d, pl.ds(0, BR)],
            head_ref.at[dest, pl.ds(pl.multiple_of((i * SLOTS + s) * BR, BR), BR)],
            head_sem,
        ).start()
        for k, out in ((0, tail0_ref), (1, tail1_ref)):
            @pl.when(i == k)
            def _():
                pltpu.make_async_copy(
                    stage.at[d, pl.ds(BR, 2 * BR)], out.at[dest, s], tail_sem
                ).start()
        return carry

    for k in range(parts):
        load(k).wait()
        lax.fori_loop(k * step, (k + 1) * step, route, 0)

    lane = lax.broadcasted_iota(jnp.int32, (META, 128), 1)

    def describe(dest, carry):
        row = jnp.zeros((META, 128), jnp.int32)
        for t in range(2 * SLOTS):
            for f in range(3):
                row = jnp.where(lane == t * 3 + f, codes[(dest * 2 * SLOTS + t) * 4 + f], row)
        meta[dest] = row.astype(jnp.float32).astype(jnp.bfloat16)
        return carry

    lax.fori_loop(0, PLANE, describe, 0)

    heads = stage.at[:, pl.ds(0, BR)]
    pltpu.make_async_copy(heads, heads, head_sem).wait()
    described = pltpu.make_async_copy(
        meta, head_ref.at[:, pl.ds(2 * SLOTS * BR, META)], meta_sem
    )
    described.start()
    tails = stage.at[:, pl.ds(BR, 2 * BR)]
    pltpu.make_async_copy(tails, tails, tail_sem).wait()
    described.wait()


def pack(row_map, anc_order, anc_below, desc_panel):
    smem = pl.BlockSpec(memory_space=pltpu.SMEM)
    hbm = pl.BlockSpec(memory_space=pltpu.HBM)
    dt = desc_panel.dtype
    return pl.pallas_call(
        pack_kernel,
        out_shape=(
            jax.ShapeDtypeStruct((PLANE, HEAD_ROWS, BR), dt),
            jax.ShapeDtypeStruct((PLANE, SLOTS, 2 * BR, BR), dt),
            jax.ShapeDtypeStruct((PLANE, SLOTS, 2 * BR, BR), dt),
        ),
        in_specs=[smem, smem, smem, hbm],
        out_specs=(hbm, hbm, hbm),
        scratch_shapes=[
            pltpu.VMEM(desc_panel.shape, dt),
            pltpu.VMEM((PLANE, META, BR), dt),
            pltpu.SMEM((NA,), jnp.int32),
            pltpu.SMEM((NA,), jnp.int32),
            pltpu.SMEM((NA * SLOTS * 4,), jnp.int32),
            pltpu.SemaphoreType.DMA((4,)),
            pltpu.SemaphoreType.DMA,
            pltpu.SemaphoreType.DMA,
            pltpu.SemaphoreType.DMA,
        ],
        name="pack",
    )(row_map.T, anc_order, anc_below.T, desc_panel)


GROUP = 16
BELOW_GROUP = 16


def diag_kernel(codes, head_ref, out_ref):
    step = pl.program_id(0)

    @pl.when(step == 0)
    def _():
        out_ref[...] = jnp.zeros_like(out_ref)

    for g in range(GROUP):
        blocks = [head_ref[g, t * BR:(t + 1) * BR, :] for t in range(2 * SLOTS)]
        products = [nt_dot(block, block) for block in blocks]
        for t, product in enumerate(products):
            c = codes[step * GROUP + g, t * 3]
            place = jnp.where(c < CB, (t // SLOTS) * CB + c, 2 * CB)
            out_ref[place] = out_ref[place] + product


def diag_sums(codes, head):
    return pl.pallas_call(
        diag_kernel,
        out_shape=jax.ShapeDtypeStruct((2 * CB + 1, BR, BR), jnp.float32),
        grid_spec=pltpu.PrefetchScalarGridSpec(
            num_scalar_prefetch=1,
            grid=(PLANE // GROUP,),
            in_specs=[pl.BlockSpec((GROUP, HEAD_ROWS, BR), lambda k, codes: (k, 0, 0))],
            out_specs=pl.BlockSpec((2 * CB + 1, BR, BR), lambda k, codes: (0, 0, 0)),
        ),
        name="diag_sums",
    )(codes, head)


def below_kernel(i, codes, head_ref, tail_ref, out_ref):
    step = pl.program_id(0)

    @pl.when(step == 0)
    def _():
        out_ref[...] = jnp.zeros_like(out_ref)

    for g in range(BELOW_GROUP):
        products = [
            nt_dot(tail_ref[g, s], head_ref[g, s * BR:(s + 1) * BR, :]) for s in range(SLOTS)
        ]
        for s, product in enumerate(products):
            t = i * SLOTS + s
            c = codes[step * BELOW_GROUP + g, t * 3]
            for r in range(2):
                j = codes[step * BELOW_GROUP + g, t * 3 + 1 + r]
                place = ((j % Y) * (Q // Y) + j // Y) * CB + c
                place = jnp.where(c < CB, place, BELOW)
                out_ref[place] = out_ref[place] + product[r * BR:(r + 1) * BR]


def below_sums(i, codes, head, tail):
    return pl.pallas_call(
        functools.partial(below_kernel, i),
        out_shape=jax.ShapeDtypeStruct((BELOW + PIECE, BR, BR), jnp.float32),
        grid_spec=pltpu.PrefetchScalarGridSpec(
            num_scalar_prefetch=1,
            grid=(PLANE // BELOW_GROUP,),
            in_specs=[
                pl.BlockSpec((BELOW_GROUP, SLOTS * BR, BR), lambda k, codes: (k, i, 0)),
                pl.BlockSpec((BELOW_GROUP, SLOTS, 2 * BR, BR), lambda k, codes: (k, 0, 0, 0)),
            ],
            out_specs=pl.BlockSpec((BELOW + PIECE, BR, BR), lambda k, codes: (0, 0, 0)),
        ),
    )(codes, head, tail)


def nn_dot(a, b):
    return lax.dot_general(
        a, b, (((1,), (0,)), ((), ())), precision=HIGHEST, preferred_element_type=jnp.float32
    )


def tn_dot(a, b):
    return lax.dot_general(
        a, b, (((0,), (0,)), ((), ())), precision=HIGHEST, preferred_element_type=jnp.float32
    )


def factor_block(pair, between):
    sub = lax.broadcasted_iota(jnp.int32, (NB, BR), 0)
    sub2 = lax.broadcasted_iota(jnp.int32, (NB, 2 * BR), 0)
    lane = lax.broadcasted_iota(jnp.int32, (NB, BR), 1)
    for k in range(BR // NB):
        between(k)
        rows = pair[k * NB:(k + 1) * NB, :]
        cols = [jnp.broadcast_to(rows[:, k * NB + j:k * NB + j + 1], (NB, BR)) for j in range(NB)]
        for j in range(NB):
            scale = lax.rsqrt(cols[j][j:j + 1, :])
            column = cols[j] * scale
            below = jnp.where(sub > j, column, 0.0)
            row = rows[j:j + 1, :] * jnp.concatenate([scale, scale], axis=1)
            rows = jnp.where(sub2 == j, row, rows - jnp.concatenate([below, below], axis=1) * row)
            for m in range(j + 1, NB):
                cols[m] = cols[m] - below * column[m:m + 1, :]
        pair[k * NB:(k + 1) * NB, :] = rows
        start = (k + 1) * NB
        if start < BR:
            left = jnp.where(lane >= start, rows[:, :BR], 0.0)
            pair[start:, :] = pair[start:, :] - tn_dot(left, rows)[start:]


def factor_whole(lower_ref, inverse_ref, work, pair, between):
    width = work.shape[0]
    inverse_ref[...] = jnp.zeros_like(inverse_ref)
    row = lax.broadcasted_iota(jnp.int32, (BR, BR), 0)
    col = lax.broadcasted_iota(jnp.int32, (BR, BR), 1)
    all_rows = lax.broadcasted_iota(jnp.int32, (width, BR), 0)
    wide = lax.broadcasted_iota(jnp.int32, (BR, width), 1)
    high = lax.broadcasted_iota(jnp.int32, (BR, width), 0)

    def step(kb, carry):
        at = pl.ds(pl.multiple_of(kb * BR, BR), BR)
        pair[:, :BR] = work[at, at]
        pair[:, BR:] = jnp.where(row == col, 1.0, 0.0)
        factor_block(pair, functools.partial(between, kb))
        diagonal = jnp.where(col >= row, pair[:, :BR], 0.0).T
        small = jnp.where(col <= row, pair[:, BR:], 0.0)
        between(kb, BR // NB)
        panel = nt_dot(work[:, at], small, HIGHEST)
        panel = jnp.where(all_rows >= (kb + 1) * BR, panel, 0.0)
        lower_ref[:, at] = panel
        lower_ref[at, at] = diagonal
        work[...] = work[...] - nt_dot(panel, panel, HIGHEST)
        between(kb, BR // NB + 1)
        before = jnp.where(wide < kb * BR, lower_ref[at, :], 0.0)
        target = jnp.where(wide == high + kb * BR, 1.0, 0.0) - nn_dot(before, inverse_ref[...])
        inverse_ref[at, :] = nn_dot(small, target)
        return carry

    lax.fori_loop(0, width // BR, step, 0)


def remote(src, dst, send_sem, recv_sem, **device):
    return pltpu.make_async_remote_copy(
        src_ref=src, dst_ref=dst, send_sem=send_sem, recv_sem=recv_sem,
        device_id=device, device_id_type=pl.DeviceIdType.MESH,
    )


def signal(semaphore, **device):
    pl.semaphore_signal(
        semaphore, inc=1, device_id=device, device_id_type=pl.DeviceIdType.MESH
    )


def target_z(i, core, y):
    return y + Y * jnp.bitwise_xor(core, i)


def diag_reduce_kernel(sums, out, arrived, send_sems, recv_sems):
    z, y = lax.axis_index("z"), lax.axis_index("y")
    core = lax.axis_index("xc") % 2
    here = z % Y == y

    barrier = pltpu.get_barrier_semaphore()
    for source in range(Z):
        @pl.when(jnp.logical_and(here, source != z))
        def _():
            signal(barrier, z=jnp.int32(source))
    pl.semaphore_wait(barrier, 2 - here.astype(jnp.int32))

    def send(i):
        return remote(
            sums.at[pl.ds(i * CB, CB)], arrived.at[z], send_sems.at[i], recv_sems.at[z],
            z=target_z(i, core, y),
        )

    for i in range(2):
        @pl.when(target_z(i, core, y) != z)
        def _():
            send(i).start()

        @pl.when(target_z(i, core, y) == z)
        def _():
            arrived[z] = sums[i * CB:(i + 1) * CB]

    @pl.when(here)
    def _():
        for source in range(Z):
            @pl.when(source != z)
            def _():
                remote(
                    sums.at[pl.ds(0, CB)], arrived.at[source], send_sems.at[0],
                    recv_sems.at[source], z=(z + 1) % Z,
                ).wait_recv()
        update = arrived[0]
        for source in range(1, Z):
            update = update + arrived[source]
        out[...] = update

    @pl.when(jnp.logical_not(here))
    def _():
        out[...] = jnp.zeros_like(out)

    for i in range(2):
        @pl.when(target_z(i, core, y) != z)
        def _():
            send(i).wait_send()


def diag_reduce(sums):
    return pl.pallas_call(
        diag_reduce_kernel,
        out_shape=jax.ShapeDtypeStruct((CB, BR, BR), jnp.float32),
        in_specs=[IN_VMEM],
        out_specs=IN_VMEM,
        scratch_shapes=[
            pltpu.VMEM((Z, CB, BR, BR), jnp.float32),
            pltpu.SemaphoreType.DMA((2,)),
            pltpu.SemaphoreType.DMA((Z,)),
        ],
        compiler_params=pltpu.CompilerParams(collective_id=0, has_side_effects=True),
        name="diag_reduce",
    )(sums)


def spread_route(k):
    pairs = []
    for z in range(Z):
        for xc in range(XC):
            base = (z * XC + xc) * Y
            pairs.append((base + z % Y, base + (z + k) % Y))
    return pairs


class Chain:
    def __init__(self, i, sums, up, down, up_sems, down_sems, send_sem):
        self.z, self.y = lax.axis_index("z"), lax.axis_index("y")
        self.distance = (target_z(i, lax.axis_index("xc") % 2, self.y) - self.z + Z) % Z
        self.above, self.under = (self.z + 1) % Z, (self.z + Z - 1) % Z
        self.sums, self.up, self.down = sums, up, down
        self.up_sems, self.down_sems, self.send_sem = up_sems, down_sems, send_sem

    def meet(self, barrier):
        signal(barrier, z=self.above)
        signal(barrier, z=self.under)

    def copy(self, source, buffer, sems, q, to):
        return remote(source.at[q], buffer.at[q], self.send_sem, sems.at[q], z=to)

    def begin(self):
        for distance, buffer, sems, to in (
            (4, self.up, self.up_sems, self.above), (5, self.down, self.down_sems, self.under)
        ):
            @pl.when(self.distance == distance)
            def _():
                def body(q, carry):
                    self.copy(self.sums, buffer, sems, q, to).start()
                    return carry

                lax.fori_loop(0, PIECES, body, 0)

    def advance(self, q, deliver):
        for some, buffer, sems, to in (
            (jnp.logical_and(self.distance >= 1, self.distance <= 3),
             self.up, self.up_sems, self.above),
            (self.distance >= 6, self.down, self.down_sems, self.under),
        ):
            @pl.when(some)
            def _():
                self.copy(self.sums, buffer, sems, q, to).wait_recv()
                buffer[q] = buffer[q] + self.sums[q]
                self.copy(buffer, buffer, sems, q, to).start()

        @pl.when(self.distance == 0)
        def _():
            self.copy(self.sums, self.up, self.up_sems, q, self.above).wait_recv()
            self.copy(self.sums, self.down, self.down_sems, q, self.above).wait_recv()
            deliver(q, self.up[q] + self.down[q] + self.sums[q])

    def finish(self):
        @pl.when(self.distance != 0)
        def _():
            remote(self.up, self.up, self.send_sem, self.up_sems.at[0], z=self.above).wait_send()


CHAIN_SCRATCH = [
    pltpu.VMEM((PIECES, PIECE, BR, BR), jnp.float32),
    pltpu.VMEM((PIECES, PIECE, BR, BR), jnp.float32),
    pltpu.SemaphoreType.DMA((PIECES,)),
    pltpu.SemaphoreType.DMA((PIECES,)),
    pltpu.SemaphoreType.DMA,
]
IN_VMEM = pl.BlockSpec(memory_space=pltpu.VMEM)


def first_kernel(sums, total, up, down, up_sems, down_sems, send_sem):
    chain = Chain(0, sums, up, down, up_sems, down_sems, send_sem)
    barrier = pltpu.get_barrier_semaphore()
    chain.meet(barrier)
    pl.semaphore_wait(barrier, 2)
    chain.begin()

    def deliver(q, value):
        total[q] = value

    def body(q, carry):
        chain.advance(q, deliver)
        return carry

    lax.fori_loop(0, PIECES, body, 0)
    chain.finish()


def first_reduce(sums):
    return pl.pallas_call(
        first_kernel,
        out_shape=jax.ShapeDtypeStruct((PIECES, PIECE, BR, BR), jnp.float32),
        in_specs=[IN_VMEM],
        out_specs=IN_VMEM,
        scratch_shapes=CHAIN_SCRATCH,
        compiler_params=pltpu.CompilerParams(collective_id=1, has_side_effects=True),
        name="first_reduce",
    )(sums.reshape(PIECES + 1, PIECE, BR, BR))


def second_kernel(
    sums, total, strip, strip1, strip2, strip3, part, part1, part2, part3, out, lower, inverse,
    up, down, up_sems, down_sems, send_sem, final, final_sems, spread_sem, work, pair, strips,
):
    chain = Chain(1, sums, up, down, up_sems, down_sems, send_sem)
    z, y = chain.z, chain.y
    has_first = chain.distance == 4
    own = PIECES // Y
    barrier = pltpu.get_barrier_semaphore()
    chain.meet(barrier)
    for k in range(1, Y):
        signal(barrier, y=(y + k) % Y)
    pl.semaphore_wait(barrier, Y + 1)
    chain.begin()

    def spread(source, q):
        return remote(source.at[q], final.at[q % own], spread_sem, final_sems.at[q % own], y=q // own)

    @pl.when(has_first)
    def _():
        def body(q, carry):
            @pl.when(q // own == y)
            def _():
                out[q % own] = total[q]

            @pl.when(q // own != y)
            def _():
                spread(total, q).start()

            return carry

        lax.fori_loop(0, PIECES, body, 0)

    def deliver(q, value):
        @pl.when(q // own == y)
        def _():
            out[q % own] = value

        @pl.when(q // own != y)
        def _():
            up[q] = value
            spread(up, q).start()

    for k, one in enumerate((strip, strip1, strip2, strip3)):
        strips[(y + Y - k) % Y] = one[...]
    work[...] = jnp.zeros_like(work)
    blocks = {(1, 0): strips[1, 0], (2, 1): strips[2, 0], (3, 2): strips[3, 0],
              (3, 0): strips[0, 0].T, (2, 0): strips[2, 1], (3, 1): strips[3, 1]}
    for c in range(CB):
        blocks[c, c] = strips[c, 2] - (part[c] + part1[c] + part2[c] + part3[c])
    for (b, c), block in blocks.items():
        work[b * BR:(b + 1) * BR, c * BR:(c + 1) * BR] = block

    turns = (2, 1, 1, 2, 1, 1, 1, 1, 2, 2)

    def between(kb, k):
        for n in range(turns[k]):
            q = kb * sum(turns) + sum(turns[:k]) + n

            @pl.when(q < PIECES)
            def _():
                chain.advance(q, deliver)

    factor_whole(lower, inverse, work, pair, between)
    chain.finish()

    @pl.when(z % Y == y)
    def _():
        part = up.at[pl.ds(0, PIECES - own)]
        remote(part, part, spread_sem, up_sems.at[0], z=chain.above).wait_send()

    @pl.when(z % Y != y)
    def _():
        def body(place, carry):
            chain.copy(sums, final, final_sems, place, chain.above).wait_recv()
            out[place] = final[place]
            return carry

        lax.fori_loop(0, own, body, 0)


def second_reduce(sums, total, strips, parts):
    own, width = PIECES // Y, CB * BR
    square = jax.ShapeDtypeStruct((width, width), jnp.float32)
    return pl.pallas_call(
        second_kernel,
        out_shape=(jax.ShapeDtypeStruct((own, PIECE, BR, BR), jnp.float32), square, square),
        in_specs=[IN_VMEM] * (2 + 2 * Y),
        out_specs=(IN_VMEM,) * 3,
        scratch_shapes=CHAIN_SCRATCH + [
            pltpu.VMEM((own, PIECE, BR, BR), jnp.float32),
            pltpu.SemaphoreType.DMA((own,)),
            pltpu.SemaphoreType.DMA,
            pltpu.VMEM((width, width), jnp.float32),
            pltpu.VMEM((BR, 2 * BR), jnp.float32),
            pltpu.VMEM((Y, 3, BR, BR), jnp.float32),
        ],
        compiler_params=pltpu.CompilerParams(collective_id=2, has_side_effects=True),
        name="second_reduce",
    )(sums.reshape(PIECES + 1, PIECE, BR, BR), total, *strips, *parts)


def solve_kernel(y_ref, rows_ref, lower_ref, inverse_ref, update_ref, out_ref):
    m = pl.program_id(0)

    @pl.when(m == 0)
    def _():
        out_ref[0, 0, 0] = lower_ref[...]

    @pl.when(m > 0)
    def _():
        update = jnp.concatenate([update_ref[0, c] for c in range(CB)], axis=1)
        out_ref[0, 0, 0] = nt_dot(rows_ref[0, 0, 0] - update, inverse_ref[...], HIGHEST)


def solve(anc_panel, lower, inverse, update, y):
    width = anc_panel.shape[4]
    update = update.reshape(Q // Y, CB, BR, BR)
    return pl.pallas_call(
        solve_kernel,
        out_shape=jax.ShapeDtypeStruct(anc_panel.shape, jnp.float32),
        grid_spec=pltpu.PrefetchScalarGridSpec(
            num_scalar_prefetch=1,
            grid=(anc_panel.shape[1],),
            in_specs=[
                pl.BlockSpec((1, 1, 1, BR, width), lambda m, y: (0, m, 0, 0, 0)),
                pl.BlockSpec((BR, width), lambda m, y: (y[0], 0)),
                pl.BlockSpec((width, width), lambda m, y: (0, 0)),
                pl.BlockSpec((1, CB, BR, BR), lambda m, y: (jnp.maximum(m - 1, 0), 0, 0, 0)),
            ],
            out_specs=pl.BlockSpec((1, 1, 1, BR, width), lambda m, y: (0, m, 0, 0, 0)),
        ),
        name="solve",
    )(y, anc_panel, lower, inverse, update)


def exchange(value):
    return lax.all_to_all(value, ("xc", "y"), split_axis=0, concat_axis=0, tiled=True)


def strip_blocks(anc_panel, y):
    strip = anc_panel[0, 0, 0]
    columns = [lax.rem(y + Y - 1, Y), lax.rem(y + 2, Y), y]
    zero = jnp.int32(0)
    return jnp.stack(
        [lax.dynamic_slice(strip, (zero, c * BR), (BR, BR), allow_negative_indices=False) for c in columns]
    )


def shards(desc_panel, row_map, anc_order, anc_below, anc_panel):
    y = lax.axis_index("y").astype(jnp.int32)
    head, tail0, tail1 = pack(row_map, anc_order, anc_below, desc_panel)
    head = exchange(head)
    tail0, head, anc_panel = lax.optimization_barrier((tail0, head, anc_panel))
    tail0 = exchange(tail0)
    codes = head[:, 2 * SLOTS * BR, : 2 * SLOTS * 3].astype(jnp.int32)
    part = diag_reduce(diag_sums(codes, head))
    strip = strip_blocks(anc_panel, y)
    strips, parts = [strip], [part]
    for k in range(1, Y):
        strips.append(lax.ppermute(strip, "y", [(b, (b + k) % Y) for b in range(Y)]))
    for k in range(1, Y):
        parts.append(lax.ppermute(part, ALL, spread_route(k)))
    tail1, tail0, part = lax.optimization_barrier((tail1, tail0, part))
    tail1 = exchange(tail1)
    total = first_reduce(below_sums(0, codes, head, tail0))
    tail1, total = lax.optimization_barrier((tail1, total))
    sums = below_sums(1, codes, head, tail1)
    update, lower, inverse = second_reduce(sums, total, strips, parts)
    return solve(anc_panel, lower, inverse, update, y.reshape(1))


def solution(mesh):
    grid = Mesh(mesh.devices.reshape(Z, XC, Y), ALL)
    in_specs = (
        P(ALL, None, None),
        P(ALL, None),
        P(),
        P(),
        P(("z", "xc"), None, "y", None, None),
    )
    out_specs = P(("z", "xc"), None, "y", None, None)
    return jax.shard_map(
        shards, mesh=grid, in_specs=in_specs, out_specs=out_specs, check_vma=False
    )
```
